32 devices in a mesh: data: 32 (over z, y, x, core).
Axes of the slice: x: 2, y: 2, z: 4, core: 2. Of those that a mesh axis runs over, the one named last changes fastest.
Arguments:
- act_in: bfloat16 [16384, 2560], P('data')
- grad_out: bfloat16 [16384, 2560], P('data')
- w_up: bfloat16 [2, 2560, 6912], replicated
- w_down: bfloat16 [2, 6912, 2560], replicated
- q_up: bfloat16 [2, 6912, 512], replicated
- q_down: bfloat16 [2, 2560, 512], replicated
Outputs:
- output 1: bfloat16 [2, 2560, 6912], replicated
- output 2: bfloat16 [2, 6912, 2560], replicated
- output 3: float32 [2, 6912, 512], replicated
- output 4: float32 [2, 2560, 512], replicated
All inputs are finite; a program needn't handle non-finite values.
Results may differ from the reference program's by a relative error of at most 0.00803997.
Values are sent between devices in bfloat16 or wider.
A program may use at most 1.5 GiB of HBM per device.

```python
import math
import jax
import jax.numpy as jnp
from jax import lax

DATA = 32
TOK = 512
D = 2560
FF = 6912
RANK = 512
LAYERS = 2

TOKENS = TOK * DATA
STEP_SIZE = 0.4 / math.sqrt(RANK)


def setup_inputs(seed: int = 0) -> dict:
    rng_key = jax.random.key(seed)
    sub_keys = jax.random.split(rng_key, 6)
    tok_rows = jax.random.normal(sub_keys[0], (TOKENS, D), jnp.float32)
    grad_rows = jax.random.normal(sub_keys[1], (TOKENS, D), jnp.float32) * (TOKENS ** -0.5)
    w_up = jax.random.normal(sub_keys[2], (LAYERS, D, FF), jnp.float32) * (D ** -0.5)
    w_down = jax.random.normal(sub_keys[3], (LAYERS, FF, D), jnp.float32) * (FF ** -0.5)
    q_up = jax.random.normal(sub_keys[4], (LAYERS, FF, RANK), jnp.float32) * (FF ** -0.5)
    q_down = jax.random.normal(sub_keys[5], (LAYERS, D, RANK), jnp.float32) * (D ** -0.5)
    return {"act_in": tok_rows.astype(jnp.bfloat16), "grad_out": grad_rows.astype(jnp.bfloat16), "w_up": w_up.astype(jnp.bfloat16), "w_down": w_down.astype(jnp.bfloat16), "q_up": q_up.astype(jnp.bfloat16), "q_down": q_down.astype(jnp.bfloat16)}


def gelu_tanh(values):
    return jax.nn.gelu(values, approximate=True)


def gelu_grad(pre_gelu, cot_gelu):
    pull_back = jax.vjp(gelu_tanh, pre_gelu)[1]
    return pull_back(cot_gelu)[0]


def mat_nn(left_op, right_op):
    return jnp.dot(left_op, right_op, preferred_element_type=jnp.float32)


def mat_nt(left_op, right_op):
    return lax.dot_general(left_op, right_op, (((1,), (1,)), ((), ())), preferred_element_type=jnp.float32)


def mat_tn(left_op, right_op):
    return lax.dot_general(left_op, right_op, (((0,), (0,)), ((), ())), preferred_element_type=jnp.float32)


def block_pairs(tok_rows, grad_rows, w_up, w_down):
    hiddens = []
    pre_gelus = []
    gelu_outs = []
    hidden = tok_rows
    for layer in range(LAYERS):
        hiddens.append(hidden)
        pre_gelu = mat_nn(hidden, w_up[layer]).astype(jnp.bfloat16)
        gelu_out = gelu_tanh(pre_gelu.astype(jnp.float32)).astype(jnp.bfloat16)
        pre_gelus.append(pre_gelu)
        gelu_outs.append(gelu_out)
        if layer + 1 < LAYERS:
            hidden = (hidden.astype(jnp.float32) + mat_nn(gelu_out, w_down[layer])).astype(jnp.bfloat16)
    up_pairs = [None] * LAYERS
    down_pairs = [None] * LAYERS
    cot_hidden = grad_rows
    for layer in reversed(range(LAYERS)):
        down_pairs[layer] = (gelu_outs[layer], cot_hidden)
        cot_gelu = mat_nt(cot_hidden, w_down[layer])
        cot_pre = gelu_grad(pre_gelus[layer].astype(jnp.float32), cot_gelu).astype(jnp.bfloat16)
        up_pairs[layer] = (hiddens[layer], cot_pre)
        if layer > 0:
            cot_hidden = (cot_hidden.astype(jnp.float32) + mat_nt(cot_pre, w_up[layer])).astype(jnp.bfloat16)
    return up_pairs, down_pairs


def left_term(row_pair, q_fac):
    left_in, right_in = row_pair
    sketch = mat_nn(right_in, q_fac).astype(jnp.bfloat16)
    return mat_tn(left_in, sketch)


def right_term(row_pair, p_hat):
    left_in, right_in = row_pair
    back_in = mat_nn(left_in, p_hat).astype(jnp.bfloat16)
    return mat_tn(right_in, back_in)


def col_normalise(p_sum):
    return (p_sum / jnp.sqrt(jnp.sum(p_sum * p_sum, axis=-2, keepdims=True))).astype(jnp.bfloat16)


def apply_update(weight, p_hat, q_sum):
    return (weight.astype(jnp.float32) - STEP_SIZE * mat_nt(p_hat, q_sum.astype(jnp.bfloat16))).astype(jnp.bfloat16)


def reference(act_in, grad_out, w_up, w_down, q_up, q_down):
    blocks = (act_in.reshape(DATA, TOK, D), grad_out.reshape(DATA, TOK, D))

    def left_pass(totals, block_pair):
        up_pairs, down_pairs = block_pairs(block_pair[0], block_pair[1], w_up, w_down)
        up_part = jnp.stack([left_term(up_pairs[layer], q_up[layer]) for layer in range(LAYERS)])
        down_part = jnp.stack([left_term(down_pairs[layer], q_down[layer]) for layer in range(LAYERS)])
        return (totals[0] + up_part, totals[1] + down_part), None

    left_zero = (jnp.zeros((LAYERS, D, RANK), jnp.float32), jnp.zeros((LAYERS, FF, RANK), jnp.float32))
    left_sums = lax.scan(left_pass, left_zero, blocks)[0]
    p_hat_up = col_normalise(left_sums[0])
    p_hat_down = col_normalise(left_sums[1])

    def right_pass(totals, block_pair):
        up_pairs, down_pairs = block_pairs(block_pair[0], block_pair[1], w_up, w_down)
        up_part = jnp.stack([right_term(up_pairs[layer], p_hat_up[layer]) for layer in range(LAYERS)])
        down_part = jnp.stack([right_term(down_pairs[layer], p_hat_down[layer]) for layer in range(LAYERS)])
        return (totals[0] + up_part, totals[1] + down_part), None

    right_zero = (jnp.zeros((LAYERS, FF, RANK), jnp.float32), jnp.zeros((LAYERS, D, RANK), jnp.float32))
    q_up_new, q_down_new = lax.scan(right_pass, right_zero, blocks)[0]
    w_up_new = jnp.stack([apply_update(w_up[layer], p_hat_up[layer], q_up_new[layer]) for layer in range(LAYERS)])
    w_down_new = jnp.stack([apply_update(w_down[layer], p_hat_down[layer], q_down_new[layer]) for layer in range(LAYERS)])
    return (w_up_new, w_down_new, q_up_new, q_down_new)
```

```python
import math
import functools
import jax
import jax.numpy as jnp
from jax import lax
from jax.experimental import pallas as pl
from jax.experimental.pallas import tpu as pltpu

MESH = pl.DeviceIdType.MESH
CYCLES = (
    (0, 1, 3, 2, 6, 7, 5, 9, 11, 10, 14, 15, 13, 12, 8, 4),
    (0, 1, 5, 4, 6, 10, 8, 9, 13, 12, 14, 15, 11, 7, 3, 2),
    (0, 2, 6, 7, 3, 1, 5, 9, 13, 15, 11, 10, 14, 12, 8, 4),
)
RINGS = tuple((j, d) for j in range(3) for d in range(2))
CHIPS = 16


def pick(table, index):
    value = jnp.int32(table[0])
    for k in range(1, len(table)):
        value = jnp.where(index == k, jnp.int32(table[k]), value)
    return value


def inverse(table):
    return tuple(table.index(k) for k in range(len(table)))


class Place:
    def __init__(self):
        me = lax.axis_index("data")
        self.core = lax.rem(me, 2)
        self.chip = lax.div(me, 2)
        self.partner = me + 1 - 2 * self.core
        self.pos = [pick(inverse(c), self.chip) for c in CYCLES]
        self.ahead = [2 * pick(c, lax.rem(p + 1, CHIPS)) + self.core for c, p in zip(CYCLES, self.pos)]
        self.behind = [2 * pick(c, lax.rem(p + CHIPS - 1, CHIPS)) + self.core for c, p in zip(CYCLES, self.pos)]

    def target(self, j, d):
        return self.ahead[j] if d == 0 else self.behind[j]

    def owner(self, j, d, back):
        p = self.pos[j]
        index = lax.rem(p + 2 * CHIPS - back, CHIPS) if d == 0 else lax.rem(p + back, CHIPS)
        return pick(CYCLES[j], index)

    def barrier(self):
        sem = pltpu.get_barrier_semaphore()
        for dev in (*self.ahead, *self.behind, self.partner):
            pl.semaphore_signal(sem, inc=1, device_id=(dev,), device_id_type=MESH)
        pl.semaphore_wait(sem, 7)


def remote(src, dst, send, recv, dev):
    return pltpu.make_async_remote_copy(src_ref=src, dst_ref=dst, send_sem=send, recv_sem=recv, device_id=(dev,), device_id_type=MESH)


def drain(ref, sem):
    pltpu.make_async_copy(ref, ref, sem).wait()


AHEAD = 3


def left_kernel(m1, m2, p1_ref, p2_ref, o1_ref, o2_ref, mine, part, slots, phat, stage_sem, pair_send, pair_recv, ring_send, ring_recv, gat_send, gat_recv, fwd_send, fwd_recv, out_sem):
    width = m1 + m2
    tiles = width // 128
    third = (tiles + 2) // 3 * 128
    cuts = (0, third, 2 * third, width)
    spans = tuple((cuts[j], cuts[j + 1] - cuts[j]) for j in range(3))
    here = Place()
    here.barrier()

    def pieces(j):
        start, size = spans[j]
        out = []
        if start < m1:
            out.append((p1_ref, start, start, min(size, m1 - start)))
        if start + size > m1:
            first = max(start, m1)
            out.append((p2_ref, first - m1, first, start + size - first))
        return out

    def stage(t):
        for j, d in RINGS:
            row = 16 * here.owner(j, d, t + 1) + 8 * d
            for ref, col, place, size in pieces(j):
                to = pl.ds(place, size)
                frm = pl.ds(col, size)
                pltpu.make_async_copy(ref.at[pl.ds(256 * here.core + row, 8), frm], mine.at[pl.ds(row, 8), to], stage_sem.at[t]).start()
                remote(ref.at[pl.ds(256 * (1 - here.core) + row, 8), frm], part.at[pl.ds(row, 8), to], pair_send.at[t], pair_recv.at[t], here.partner).start()

    def step(t, first, last):
        drain(mine.at[pl.ds(0, 16)], stage_sem.at[t])
        drain(part.at[pl.ds(0, 16)], pair_recv.at[t])
        for r, (j, d) in enumerate(RINGS):
            start, size = spans[j]
            row = 16 * here.owner(j, d, t + 1) + 8 * d
            block = mine.at[pl.ds(row, 8), pl.ds(start, size)]
            value = block[...] + part[pl.ds(row, 8), pl.ds(start, size)]
            if not first:
                slot = slots.at[t - 1, r, :, pl.ds(0, size)]
                drain(slot, ring_recv.at[t - 1, r])
                value = value + slot[...]
            block[...] = value
            if not last:
                remote(block, slots.at[t, r, :, pl.ds(0, size)], ring_send.at[t], ring_recv.at[t, r], here.target(j, d)).start()

    for t in range(AHEAD):
        stage(t)
    stage(AHEAD)
    step(0, True, False)

    def middle(t, carry):
        stage(t + AHEAD)
        step(t, False, False)
        return carry

    lax.fori_loop(1, CHIPS - AHEAD, middle, 0)
    lax.fori_loop(CHIPS - AHEAD, CHIPS - 1, lambda t, c: (step(t, False, False), c)[1], 0)
    step(CHIPS - 1, False, True)

    base = pl.multiple_of(16 * here.chip, 16)
    rows = pl.multiple_of(256 * here.core + base, 16)
    for lo, hi in ((0, m1), (m1, width)):
        total = jnp.zeros((16, 128), jnp.float32)
        for c in range(lo, hi, 128):
            v = mine[pl.ds(base, 16), pl.ds(c, 128)]
            total = total + v * v
        norm = jnp.sqrt(jnp.sum(total, axis=1, keepdims=True))
        for c in range(lo, hi, 256):
            phat[pl.ds(rows, 16), pl.ds(c, 256)] = (mine[pl.ds(base, 16), pl.ds(c, 256)] / norm).astype(jnp.bfloat16)

    group = (tiles + 5) // 6
    counts = [group if g < tiles - 6 * (group - 1) else group - 1 for g in range(6)]
    starts = [128 * sum(counts[:g]) for g in range(6)]

    def forward(row, cols, s, j, d, r, onward):
        block = phat.at[pl.ds(row, 16), cols]
        if onward:
            remote(block, block, gat_send.at[s], gat_recv.at[s, r], here.target(j, d)).start()
        remote(block, block, fwd_send.at[s], fwd_recv.at[s], here.partner).start()

    def gather_step(s, first, last):
        for r, (j, d) in enumerate(RINGS):
            row = pl.multiple_of(256 * here.core + 16 * here.owner(j, d, s), 16)
            cols = pl.ds(starts[r], 128 * counts[r])
            if not first:
                drain(phat.at[pl.ds(row, 16), cols], gat_recv.at[s - 1, r])
            forward(row, cols, s, j, d, r, not last)

    gather_step(0, True, False)
    lax.fori_loop(1, CHIPS - 1, lambda s, c: (gather_step(s, False, False), c)[1], 0)
    gather_step(CHIPS - 1, False, True)

    def flush_in(s, carry):
        drain(phat.at[pl.ds(0, 16)], fwd_recv.at[s])
        return carry

    lax.fori_loop(0, CHIPS, flush_in, 0)
    out1 = pltpu.make_async_copy(phat.at[:, pl.ds(0, m1)], o1_ref, out_sem.at[0])
    out2 = pltpu.make_async_copy(phat.at[:, pl.ds(m1, m2)], o2_ref, out_sem.at[1])
    out1.start()
    out2.start()

    def settle(s, carry):
        drain(mine.at[pl.ds(0, 16)], pair_send.at[s])
        drain(phat.at[pl.ds(0, 16)], fwd_send.at[s])
        return carry

    lax.fori_loop(0, CHIPS, settle, 0)

    def settle_rings(s, carry):
        drain(mine.at[pl.ds(0, 16)], ring_send.at[s])
        drain(phat.at[pl.ds(0, 16)], gat_send.at[s])
        return carry

    lax.fori_loop(0, CHIPS - 1, settle_rings, 0)
    out1.wait()
    out2.wait()


def left_exchange(p1, p2):
    rank, m1 = p1.shape
    m2 = p2.shape[1]
    width = m1 + m2
    third = (width // 128 + 2) // 3 * 128
    dma = pltpu.SemaphoreType.DMA
    return pl.pallas_call(
        functools.partial(left_kernel, m1, m2),
        out_shape=(jax.ShapeDtypeStruct((rank, m1), jnp.bfloat16), jax.ShapeDtypeStruct((rank, m2), jnp.bfloat16)),
        in_specs=[pl.BlockSpec(memory_space=pl.ANY)] * 2,
        out_specs=(pl.BlockSpec(memory_space=pl.ANY),) * 2,
        scratch_shapes=[
            pltpu.VMEM((256, width), jnp.float32),
            pltpu.VMEM((256, width), jnp.float32),
            pltpu.VMEM((15, 6, 8, third), jnp.float32),
            pltpu.VMEM((512, width), jnp.bfloat16),
            dma((16,)), dma((16,)), dma((16,)), dma((15,)), dma((15, 6)), dma((15,)), dma((15, 6)), dma((16,)), dma((16,)), dma((2,)),
        ],
        compiler_params=pltpu.CompilerParams(collective_id=0, has_side_effects=True, vmem_limit_bytes=60 * 2**20),
        name="left_exchange",
    )(p1, p2)


def right_kernel(n1, n2, q1_ref, q2_ref, o1_ref, o2_ref, mine, part, slots, stage_sem, pair_send, pair_recv, ring_send, ring_recv, gat_send, gat_recv, fwd_send, fwd_recv, out_sem):
    u1, u2 = n1 // 32, n2 // 32
    unit = u1 + u2
    w1 = u1 // 3
    second = (u2 - 16) // 16 * 8
    w2 = (u2 - 2 * second, second, second)
    from2 = (0, w2[0], w2[0] + second)
    sizes = tuple(w1 + w2[j] for j in range(3))
    offs = (0, sizes[0], sizes[0] + sizes[1])
    here = Place()
    here.barrier()

    def pieces(core, chip, j, d):
        base = unit * chip + offs[j]
        cols = pl.ds(256 * d, 256)
        row1 = pl.multiple_of((n1 // 2) * core + u1 * chip + w1 * j, 8)
        row2 = pl.multiple_of((n2 // 2) * core + u2 * chip + from2[j], 8)
        return (
            (0, (pl.ds(row1, w1), cols), (pl.ds(pl.multiple_of(base, 8), w1), cols)),
            (1, (pl.ds(row2, w2[j]), cols), (pl.ds(pl.multiple_of(base + w1, 8), w2[j]), cols)),
        )

    ins = (q1_ref, q2_ref)
    outs = (o1_ref, o2_ref)

    def stage(t):
        for j, d in RINGS:
            chip = here.owner(j, d, t + 1)
            for k, frm, to in pieces(here.core, chip, j, d):
                pltpu.make_async_copy(ins[k].at[frm], mine.at[to], stage_sem.at[t]).start()
            for k, frm, to in pieces(1 - here.core, chip, j, d):
                remote(ins[k].at[frm], part.at[to], pair_send.at[t], pair_recv.at[t], here.partner).start()

    def step(t, first, last):
        drain(mine.at[pl.ds(0, unit)], stage_sem.at[t])
        drain(part.at[pl.ds(0, unit)], pair_recv.at[t])
        for r, (j, d) in enumerate(RINGS):
            rows = pl.ds(pl.multiple_of(unit * here.owner(j, d, t + 1) + offs[j], 8), sizes[j])
            cols = pl.ds(256 * d, 256)
            block = mine.at[rows, cols]
            value = block[...] + part[rows, cols]
            if not first:
                slot = slots.at[t - 1, r, pl.ds(0, sizes[j])]
                drain(slot, ring_recv.at[t - 1, r])
                value = value + slot[...]
            block[...] = value
            if not last:
                remote(block, slots.at[t, r, pl.ds(0, sizes[j])], ring_send.at[t], ring_recv.at[t, r], here.target(j, d)).start()

    for t in range(AHEAD):
        stage(t)
    stage(AHEAD)
    step(0, True, False)

    def middle(t, carry):
        stage(t + AHEAD)
        step(t, False, False)
        return carry

    lax.fori_loop(1, CHIPS - AHEAD, middle, 0)
    lax.fori_loop(CHIPS - AHEAD, CHIPS - 1, lambda t, c: (step(t, False, False), c)[1], 0)
    step(CHIPS - 1, False, True)

    def gather_step(s, first, last):
        for r, (j, d) in enumerate(RINGS):
            cols = pl.ds(256 * d, 256)
            if not first:
                drain(mine.at[pl.ds(0, sizes[j]), cols], gat_recv.at[s - 1, r])
            for k, to, frm in pieces(here.core, here.owner(j, d, s), j, d):
                src = mine.at[frm] if first else outs[k].at[to]
                dst = outs[k].at[to]
                if first:
                    pltpu.make_async_copy(src, dst, out_sem.at[0]).start()
                if not last:
                    remote(src, dst, gat_send.at[s], gat_recv.at[s, r], here.target(j, d)).start()
                remote(src, dst, fwd_send.at[s], fwd_recv.at[s], here.partner).start()

    gather_step(0, True, False)
    lax.fori_loop(1, CHIPS - 1, lambda s, c: (gather_step(s, False, False), c)[1], 0)
    gather_step(CHIPS - 1, False, True)

    def settle(s, carry):
        drain(mine.at[pl.ds(0, unit)], fwd_recv.at[s])
        drain(mine.at[pl.ds(0, unit)], pair_send.at[s])
        drain(mine.at[pl.ds(0, unit)], fwd_send.at[s])
        return carry

    lax.fori_loop(0, CHIPS, settle, 0)

    def settle_rings(s, carry):
        drain(mine.at[pl.ds(0, unit)], ring_send.at[s])
        drain(mine.at[pl.ds(0, unit)], gat_send.at[s])
        return carry

    lax.fori_loop(0, CHIPS - 1, settle_rings, 0)
    drain(mine.at[pl.ds(0, unit)], out_sem.at[0])


def right_exchange(q1, q2):
    n1, rank = q1.shape
    n2 = q2.shape[0]
    unit = (n1 + n2) // 32
    dma = pltpu.SemaphoreType.DMA
    return pl.pallas_call(
        functools.partial(right_kernel, n1, n2),
        out_shape=(jax.ShapeDtypeStruct((n1, rank), jnp.float32), jax.ShapeDtypeStruct((n2, rank), jnp.float32)),
        in_specs=[pl.BlockSpec(memory_space=pl.ANY)] * 2,
        out_specs=(pl.BlockSpec(memory_space=pl.ANY),) * 2,
        scratch_shapes=[
            pltpu.VMEM((16 * unit, rank), jnp.float32),
            pltpu.VMEM((16 * unit, rank), jnp.float32),
            pltpu.VMEM((15, 6, 104, 256), jnp.float32),
            dma((16,)), dma((16,)), dma((16,)), dma((15,)), dma((15, 6)), dma((15,)), dma((15, 6)), dma((16,)), dma((16,)), dma((1,)),
        ],
        compiler_params=pltpu.CompilerParams(collective_id=1, has_side_effects=True, vmem_limit_bytes=60 * 2**20),
        name="right_exchange",
    )(q1, q2)


def gelu_tanh(values):
    return jax.nn.gelu(values, approximate=True)


def gelu_grad(pre_gelu, cot_gelu):
    pull_back = jax.vjp(gelu_tanh, pre_gelu)[1]
    return pull_back(cot_gelu)[0]


def mat_nn(left_op, right_op):
    return jnp.dot(left_op, right_op, preferred_element_type=jnp.float32)


def mat_nt(left_op, right_op):
    return lax.dot_general(left_op, right_op, (((1,), (1,)), ((), ())), preferred_element_type=jnp.float32)


def mat_tn(left_op, right_op):
    return lax.dot_general(left_op, right_op, (((0,), (0,)), ((), ())), preferred_element_type=jnp.float32)


def update_up_kernel(step_size, p_ref, q_ref, w_ref, *refs):
    o_ref, qo_ref, p_rows = refs[-3:]
    m = p_rows.shape[0]

    @pl.when(pl.program_id(0) == 0)
    def _():
        for i in range(0, m, 256):
            p_rows[pl.ds(i, 256)] = p_ref[:, pl.ds(i, 256)].T

    q = q_ref[...]
    qo_ref[0] = q
    q = q.astype(jnp.bfloat16)
    for i in range(0, m, 512):
        prod = mat_nt(p_rows[pl.ds(i, 512)], q)
        o_ref[0, pl.ds(i, 512)] = (w_ref[0, pl.ds(i, 512)].astype(jnp.float32) - step_size * prod).astype(jnp.bfloat16)


def update_down_kernel(step_size, p_ref, q_ref, w_ref, *refs):
    o_ref, qo_ref, q_cols = refs[-3:]
    n = q_cols.shape[1]

    @pl.when(pl.program_id(0) == 0)
    def _():
        qo_ref[0] = q_ref[...]
        for i in range(0, n, 256):
            q_cols[:, pl.ds(i, 256)] = q_ref[pl.ds(i, 256)].astype(jnp.bfloat16).T

    p = p_ref[...].T
    for i in range(0, n, 256):
        prod = mat_nn(p, q_cols[:, pl.ds(i, 256)])
        o_ref[0, :, pl.ds(i, 256)] = (w_ref[0, :, pl.ds(i, 256)].astype(jnp.float32) - step_size * prod).astype(jnp.bfloat16)


def update(up, p_hat, q_sum, weights, layer, prev, step_size, block):
    layers, m, n = weights.shape
    rank = p_hat.shape[0]
    if up:
        grid = n // block
        w_spec = pl.BlockSpec((1, m, block), lambda i: (layer, 0, i))
        specs = [pl.BlockSpec((rank, m), lambda i: (0, 0)), pl.BlockSpec((block, rank), lambda i: (i, 0)), w_spec]
        q_spec = pl.BlockSpec((1, block, rank), lambda i: (layer, i, 0))
        scratch = pltpu.VMEM((m, rank), jnp.bfloat16)
    else:
        grid = m // block
        w_spec = pl.BlockSpec((1, block, n), lambda i: (layer, i, 0))
        specs = [pl.BlockSpec((rank, block), lambda i: (0, i)), pl.BlockSpec((n, rank), lambda i: (0, 0)), w_spec]
        q_spec = pl.BlockSpec((1, n, rank), lambda i: (layer, 0, 0))
        scratch = pltpu.VMEM((rank, n), jnp.bfloat16)
    args = [p_hat, q_sum, weights]
    alias = {}
    if prev is not None:
        specs += [pl.BlockSpec(memory_space=pl.ANY)] * 2
        args += prev
        alias = {3: 0, 4: 1}
    return pl.pallas_call(
        functools.partial(update_up_kernel if up else update_down_kernel, step_size),
        grid=(grid,),
        out_shape=(jax.ShapeDtypeStruct(weights.shape, jnp.bfloat16), jax.ShapeDtypeStruct((layers, n, rank), jnp.float32)),
        in_specs=specs,
        out_specs=(w_spec, q_spec),
        scratch_shapes=[scratch],
        input_output_aliases=alias,
        compiler_params=pltpu.CompilerParams(dimension_semantics=("arbitrary",), vmem_limit_bytes=60 * 2**20),
        cost_estimate=pl.CostEstimate(flops=2 * m * n * rank, bytes_accessed=4 * m * n, transcendentals=0),
        name="update_up" if up else "update_down",
    )(*args)


def solution(mesh):
    def left(right_in, left_in, q_fac):
        sketch = mat_nn(right_in, q_fac).astype(jnp.bfloat16)
        return mat_tn(sketch, left_in)

    def right(right_in, left_in, p_hat):
        back_in = mat_nt(left_in, p_hat).astype(jnp.bfloat16)
        return mat_tn(right_in, back_in)

    def local_step(tok_rows, grad_rows, w_up, w_down, q_up, q_down):
        step_size = 0.4 / math.sqrt(q_up.shape[-1])
        z0 = mat_nn(tok_rows, w_up[0]).astype(jnp.bfloat16)
        a0 = gelu_tanh(z0.astype(jnp.float32)).astype(jnp.bfloat16)
        h1 = (tok_rows.astype(jnp.float32) + mat_nn(a0, w_down[0])).astype(jnp.bfloat16)
        z1 = mat_nn(h1, w_up[1]).astype(jnp.bfloat16)
        a1 = gelu_tanh(z1.astype(jnp.float32)).astype(jnp.bfloat16)
        e1 = gelu_grad(z1.astype(jnp.float32), mat_nt(grad_rows, w_down[1])).astype(jnp.bfloat16)
        pu1, pd1 = left_exchange(left(e1, h1, q_up[1]), left(grad_rows, a1, q_down[1]))
        g1 = (grad_rows.astype(jnp.float32) + mat_nt(e1, w_up[1])).astype(jnp.bfloat16)
        e0 = gelu_grad(z0.astype(jnp.float32), mat_nt(g1, w_down[0])).astype(jnp.bfloat16)
        pu0, pd0 = left_exchange(left(e0, tok_rows, q_up[0]), left(g1, a0, q_down[0]))
        qu1, qd1 = right_exchange(right(e1, h1, pu1), right(grad_rows, a1, pd1))
        qu0, qd0 = right_exchange(right(e0, tok_rows, pu0), right(g1, a0, pd0))
        up = update(True, pu1, qu1, w_up, 1, None, step_size, 384)
        down = update(False, pd1, qd1, w_down, 1, None, step_size, 768)
        up = update(True, pu0, qu0, w_up, 0, up, step_size, 384)
        down = update(False, pd0, qd0, w_down, 0, down, step_size, 768)
        return up[0], down[0], up[1], down[1]

    from jax.sharding import PartitionSpec as P
    row_spec = P(mesh.axis_names[0], None)
    return jax.shard_map(local_step, mesh=mesh, in_specs=(row_spec, row_spec, P(), P(), P(), P()), out_specs=(P(), P(), P(), P()), check_vma=False)
```

```python
import math
import functools
import jax
import jax.numpy as jnp
from jax import lax
from jax.experimental import pallas as pl
from jax.experimental.pallas import tpu as pltpu
from jax.sharding import PartitionSpec as P

MESH = pl.DeviceIdType.MESH
DMA = pltpu.SemaphoreType.DMA
ANY = pl.BlockSpec(memory_space=pl.ANY)
F32, BF16 = jnp.float32, jnp.bfloat16
CYCLES = (
    (0, 1, 3, 2, 6, 7, 5, 9, 11, 10, 14, 15, 13, 12, 8, 4),
    (0, 1, 5, 4, 6, 10, 8, 9, 13, 12, 14, 15, 11, 7, 3, 2),
    (0, 2, 6, 7, 3, 1, 5, 9, 13, 15, 11, 10, 14, 12, 8, 4),
)
TILE, RANK, LANES = 256, 512, 128
CHIPS = 16
HALF = CHIPS // 2
WINDOW = 4
AHEAD = 2
COT_DEPTH = 2
K1_RATES = (2, 4, 1, 1, 4)
TURN_DEPTH = 3
TURN_RATE = 4


def mat_nn(left_op, right_op):
    return jnp.dot(left_op, right_op, preferred_element_type=F32)


def mat_nt(left_op, right_op):
    return lax.dot_general(left_op, right_op, (((1,), (1,)), ((), ())), preferred_element_type=F32)


def mat_tn(left_op, right_op):
    return lax.dot_general(left_op, right_op, (((0,), (0,)), ((), ())), preferred_element_type=F32)


def gelu_tanh(values):
    return jax.nn.gelu(values, approximate=True)


def gelu_grad(pre_gelu, cot_gelu):
    pull_back = jax.vjp(gelu_tanh, pre_gelu)[1]
    return pull_back(cot_gelu)[0]


def pick(table, index):
    value = jnp.int32(table[0])
    for k in range(1, len(table)):
        value = jnp.where(index == k, jnp.int32(table[k]), value)
    return value


def inverse(table):
    return tuple(table.index(k) for k in range(len(table)))


def loop(lo, hi, body):
    def run(i, carry):
        body(i)
        return carry

    lax.fori_loop(lo, hi, run, 0)


class Place:
    def __init__(self):
        me = lax.axis_index("data")
        self.core = lax.rem(me, 2)
        self.chip = lax.div(me, 2)
        self.partner = me + 1 - 2 * self.core
        self.pos = [pick(inverse(c), self.chip) for c in CYCLES]
        self.ahead = [2 * pick(c, lax.rem(p + 1, CHIPS)) + self.core for c, p in zip(CYCLES, self.pos)]
        self.behind = [2 * pick(c, lax.rem(p + CHIPS - 1, CHIPS)) + self.core for c, p in zip(CYCLES, self.pos)]

    def target(self, j, d):
        return jnp.where(d == 0, self.ahead[j], self.behind[j])

    def owner(self, j, d, back):
        p = self.pos[j]
        return pick(CYCLES[j], jnp.where(d == 0, lax.rem(p + 2 * CHIPS - back, CHIPS), lax.rem(p + 2 * CHIPS + back, CHIPS)))

    def barrier(self):
        sem = pltpu.get_barrier_semaphore()
        for dev in (*self.ahead, *self.behind, self.partner):
            pl.semaphore_signal(sem, inc=1, device_id=(dev,), device_id_type=MESH)
        pl.semaphore_wait(sem, 7)


def remote(src, dst, send, recv, dev):
    return pltpu.make_async_remote_copy(src_ref=src, dst_ref=dst, send_sem=send, recv_sem=recv, device_id=(dev,), device_id_type=MESH)


def drain(ref, sem):
    pltpu.make_async_copy(ref, ref, sem).wait()


class Phase:
    def __init__(self, count, loads, compute, stores=(), resident=(), depth=2):
        self.count, self.loads, self.compute, self.stores, self.resident, self.depth = count, loads, compute, stores, resident, depth
        self.follower = None

    def begin(self):
        for copy in self.resident:
            copy().start()
        for i in range(min(self.depth - 1, self.count)):
            for load in self.loads:
                load(i).start()

    def tile(self, i):
        if self.resident:
            @pl.when(i == 0)
            def _():
                for copy in self.resident:
                    copy().wait()

        for load in self.loads:
            load(i).wait()
        after = i + self.depth - 1

        @pl.when(after < self.count)
        def _():
            for load in self.loads:
                load(after).start()

        if self.stores:
            @pl.when(i >= self.depth)
            def _():
                for store in self.stores:
                    store(i - self.depth).wait()

        self.compute(i)
        for store in self.stores:
            store(i).start()
        if self.follower is not None:
            @pl.when(i == self.count - 1)
            def _():
                self.follower.begin()

    def end(self):
        for i in range(max(0, self.count - self.depth), self.count):
            for store in self.stores:
                store(i).wait()


class Background:
    def __init__(self, plan):
        self.plan = []
        at = 0
        for phase, rate in plan:
            slots = -(-phase.count // rate)
            self.plan.append((phase, rate, at, slots))
            at += slots
        self.slots = at
        for (one, *_), (other, *_) in zip(self.plan, self.plan[1:]):
            one.follower = other

    def begin(self):
        self.plan[0][0].begin()

    def run(self, slot):
        for phase, rate, at, slots in self.plan:
            lo = jnp.clip((slot - at) * rate, 0, phase.count)
            hi = jnp.clip((slot - at + 1) * rate, 0, phase.count)
            loop(lo, hi, phase.tile)

    def end(self, done):
        for phase, rate, at, slots in self.plan:
            lo = min(max((done - at) * rate, 0), phase.count)
            if lo < phase.count:
                loop(lo, phase.count, phase.tile)
            phase.end()


class Sums:
    def __init__(self, here, ins, pieces, region, refs):
        self.here, self.ins, self.pieces, self.region = here, ins, pieces, region
        self.mine, self.part, self.slots, self.stage_sem, self.pair_send, self.pair_recv, self.ring_send, self.ring_recv, self.credit = refs

    @staticmethod
    def scratch(height, width, slot_rows, slot_cols):
        return [
            pltpu.VMEM((WINDOW, 2, height, width), F32),
            pltpu.VMEM((WINDOW, 2, height, width), F32),
            pltpu.VMEM((HALF, 6, slot_rows, slot_cols), F32),
            DMA((HALF + 1,)), DMA((HALF + 1,)), DMA((HALF + 1,)), DMA((HALF,)), DMA((HALF, 6)), pltpu.SemaphoreType.REGULAR,
        ]

    def units(self, sem, t, single):
        drain(self.mine.at[0, 0] if single else self.mine.at[0], sem.at[t])

    def stage(self, t, kind, reuse):
        here = self.here
        w = lax.rem(t, WINDOW)
        if reuse is not None:
            self.units(self.ring_send, t - WINDOW, reuse == "far")
            pl.semaphore_wait(self.credit, 1)
        for d in range(1 if kind == "own" else 2):
            for j in range(3):
                chip = here.owner(j, d, t - HALF)
                for k, frm, to in self.pieces(here.core, chip, j, d, kind == "far"):
                    pltpu.make_async_copy(self.ins[k].at[frm], self.mine.at[(w, d, *to)], self.stage_sem.at[t]).start()
                for k, frm, to in self.pieces(1 - here.core, chip, j, d, kind == "far"):
                    remote(self.ins[k].at[frm], self.part.at[(w, d, *to)], self.pair_send.at[t], self.pair_recv.at[t], here.partner).start()

    def send(self, block, t, d, j, height, width):
        spot = (t, 3 * d + j, pl.ds(0, height), pl.ds(0, width))
        remote(block, self.slots.at[spot], self.ring_send.at[t], self.ring_recv.at[t, 3 * d + j], self.here.target(j, d)).start()

    def come(self, t, d, j, height, width):
        slot = self.slots.at[(t, 3 * d + j, pl.ds(0, height), pl.ds(0, width))]
        drain(slot, self.ring_recv.at[t, 3 * d + j])
        return slot

    def give(self):
        pl.semaphore_signal(self.credit, inc=1, device_id=(self.here.partner,), device_id_type=MESH)

    def start(self):
        self.stage(0, "far", None)
        self.stage(1, "full", None)
        self.stage(2, "full", None)

    def first(self):
        self.units(self.stage_sem, 0, True)
        self.units(self.pair_recv, 0, True)
        for d in range(2):
            for j in range(3):
                region = (0, d, *self.region(j, d, True))
                block = self.mine.at[region]
                value = block[...] + self.part[region]
                block[...] = value
                self.send(block, 0, d, j, *value.shape)
        self.give()

    def middle(self, t, d):
        w = lax.rem(t, WINDOW)

        @pl.when(d == 0)
        def _():
            @pl.when(t == 1)
            def _():
                self.stage(t + AHEAD, "full", None)

            @pl.when(t == 2)
            def _():
                self.stage(t + AHEAD, "full", "far")

            @pl.when((t > 2) & (t + AHEAD < HALF))
            def _():
                self.stage(t + AHEAD, "full", "full")

            @pl.when(t + AHEAD == HALF)
            def _():
                self.stage(t + AHEAD, "own", "full")

            self.units(self.stage_sem, t, False)
            self.units(self.pair_recv, t, False)

        for j in range(3):
            region = (w, d, *self.region(j, 0, False))
            block = self.mine.at[region]
            height, width = block.shape

            @pl.when(t == 1)
            def _():
                block[...] = block[...] + self.part[region]
                for side in range(2):
                    @pl.when(d == side)
                    def _():
                        half = self.region(j, side, True)
                        some = self.mine.at[(w, d, *half)]
                        slot = self.come(0, d, j, *some.shape)
                        some[...] = some[...] + slot[...]

            @pl.when(t > 1)
            def _():
                slot = self.come(t - 1, d, j, height, width)
                block[...] = block[...] + self.part[region] + slot[...]

            self.send(block, t, d, j, height, width)

        @pl.when((d == 1) & (t + WINDOW <= HALF))
        def _():
            self.give()

    def last(self):
        self.units(self.stage_sem, HALF, True)
        self.units(self.pair_recv, HALF, True)
        own = self.mine.at[HALF % WINDOW, 0]
        for j in range(3):
            region = self.region(j, 0, False)
            block = own.at[region]
            height, width = block.shape
            value = block[...] + self.part[(HALF % WINDOW, 0, *region)]
            for d in range(2):
                value = value + self.come(HALF - 1, d, j, height, width)[...]
            block[...] = value
        return own

    def run(self, hook):
        self.first()

        def body(u):
            self.middle(lax.div(u, 2), lax.rem(u, 2))
            if hook is not None:
                hook(u - 2)

        loop(2, 2 * HALF, body)
        return self.last()

    def settle(self):
        def pairs(t):
            self.units(self.pair_send, t, False)

        self.units(self.pair_send, 0, True)
        loop(1, HALF, pairs)
        self.units(self.pair_send, HALF, True)
        loop(HALF + 1 - WINDOW, HALF, lambda t: self.units(self.ring_send, t, False))


def spread(here, unit, step_fn, hook):
    step_fn(0, 0, "own")

    def body(u):
        step_fn(lax.div(u, 2), lax.rem(u, 2), "full")
        if hook is not None:
            hook(u - 2)

    loop(2, 2 * (HALF - 1), body)
    for d in range(2):
        step_fn(HALF - 1, d, "near")
    for d in range(2):
        step_fn(HALF, d, "far")


def spread_settle(unit, pair, fwd_send, fwd_recv, gat_send):
    def both(sem, s, single):
        drain(unit if single else pair, sem.at[s])

    for sem in (fwd_recv, fwd_send):
        both(sem, 0, True)
        loop(1, HALF, lambda s, sem=sem: both(sem, s, False))
        both(sem, HALF, True)
    loop(0, HALF - 1, lambda s: both(gat_send, s, False))
    both(gat_send, HALF - 1, True)


def left_sums(here, p_ref, refs):
    width = p_ref.shape[1]
    tiles = width // LANES
    third = (tiles + 2) // 3
    second = (tiles - third + 1) // 2
    cuts = (0, LANES * third, LANES * (third + second), width)

    def region(j, d, far):
        return pl.ds(8 * d if far else 0, 8 if far else 16), pl.ds(cuts[j], cuts[j + 1] - cuts[j])

    def pieces(core, chip, j, d, far):
        row = pl.multiple_of(TILE * core + 16 * chip + (8 * d if far else 0), 8)
        rows, cols = region(j, d, far)
        return ((0, (pl.ds(row, 8 if far else 16), cols), (rows, cols)),)

    return Sums(here, (p_ref,), pieces, region, refs)


def left_sums_scratch(width):
    return Sums.scratch(16, width, 16, (width // LANES + 2) // 3 * LANES)


def left_gather(here, m1, outs, refs):
    phat, gat_send, gat_recv, fwd_send, fwd_recv, out_sem = refs
    width = phat.shape[1]
    third = (width // LANES + 2) // 3 * LANES
    cuts = (0, third, 2 * third, width)

    def normalise(own, lo):
        rows = pl.ds(pl.multiple_of(TILE * here.core + 16 * here.chip, 16), 16)
        total = jnp.zeros((16, LANES), F32)
        for c in range(0, own.shape[1], LANES):
            v = own[:, pl.ds(c, LANES)]
            total = total + v * v
        norm = jnp.sqrt(jnp.sum(total, axis=1, keepdims=True))
        for c in range(0, own.shape[1], TILE):
            phat[rows, pl.ds(lo + c, TILE)] = (own[:, pl.ds(c, TILE)] / norm).astype(BF16)

    def step_fn(s, d, kind):
        for j in range(3):
            start, size = cuts[j], cuts[j + 1] - cuts[j]
            mid = (size // LANES + 1) // 2 * LANES
            halves = (pl.ds(start, mid), pl.ds(start + mid, size - mid))
            rows = pl.ds(pl.multiple_of(TILE * here.core + 16 * here.owner(j, d, s), 16), 16)
            block = phat.at[rows, pl.ds(start, size)]
            if kind == "far":
                block = phat.at[rows, halves[d]]
            if kind != "own":
                drain(block, gat_recv.at[s - 1, 3 * d + j])
            onward = ()
            if kind == "own":
                onward = ((0, block), (1, block))
            elif kind == "full":
                onward = ((d, block),)
            elif kind == "near":
                onward = ((d, phat.at[rows, halves[d]]),)
            for way, some in onward:
                remote(some, some, gat_send.at[s], gat_recv.at[s, 3 * way + j], here.target(j, way)).start()
            remote(block, block, fwd_send.at[s], fwd_recv.at[s], here.partner).start()

    def gather(hook):
        unit = phat.at[pl.ds(0, 16)]
        spread(here, unit, step_fn, hook)
        spread_settle(unit, phat.at[pl.ds(0, 32)], fwd_send, fwd_recv, gat_send)
        copies = [
            pltpu.make_async_copy(phat.at[:, pl.ds(0, m1)], outs[0], out_sem.at[0]),
            pltpu.make_async_copy(phat.at[:, pl.ds(m1, width - m1)], outs[1], out_sem.at[1]),
        ]
        for copy in copies:
            copy.start()
        return copies

    return normalise, gather


def left_gather_scratch(width):
    return [
        pltpu.VMEM((RANK, width), BF16),
        DMA((HALF,)), DMA((HALF, 6)), DMA((HALF + 1,)), DMA((HALF + 1,)), DMA((2,)),
    ]


def right_comm(here, n1, n2, ins, outs, refs):
    *sum_refs, gat_send, gat_recv, fwd_send, fwd_recv, out_sem = refs
    u1, u2 = n1 // 32, n2 // 32
    w1 = u1 // 3
    second = (u2 - 16) // 16 * 8
    w2 = (u2 - 2 * second, second, second)
    from2 = (0, w2[0], w2[0] + second)
    sizes = tuple(w1 + w2[j] for j in range(3))
    offs = (0, sizes[0], sizes[0] + sizes[1])

    def columns(d, far):
        return pl.ds(TILE * d if far else 0, TILE if far else RANK)

    def region(j, d, far):
        return pl.ds(offs[j], sizes[j]), columns(d, far)

    def pieces(core, chip, j, d, far):
        cols = columns(d, far)
        row1 = pl.multiple_of((n1 // 2) * core + u1 * chip + w1 * j, 8)
        row2 = pl.multiple_of((n2 // 2) * core + u2 * chip + from2[j], 8)
        return (
            (0, (pl.ds(row1, w1), cols), (pl.ds(offs[j], w1), cols)),
            (1, (pl.ds(row2, w2[j]), cols), (pl.ds(offs[j] + w1, w2[j]), cols)),
        )

    sums = Sums(here, ins, pieces, region, sum_refs)

    def gather(own, hook):
        def step_fn(s, d, kind):
            for j in range(3):
                chip = here.owner(j, d, s)
                if kind != "own":
                    drain(own.at[pl.ds(0, sizes[j]), columns(0, kind == "far")], gat_recv.at[s - 1, 3 * d + j])
                for k, to, frm in pieces(here.core, chip, j, d, kind == "far"):
                    dst = outs[k].at[to]
                    src = own.at[frm] if kind == "own" else dst
                    if kind == "own":
                        pltpu.make_async_copy(src, dst, out_sem.at[0]).start()
                    for way in {"own": (0, 1), "full": (d,)}.get(kind, ()):
                        remote(src, dst, gat_send.at[s], gat_recv.at[s, 3 * way + j], here.target(j, way)).start()
                    remote(src, dst, fwd_send.at[s], fwd_recv.at[s], here.partner).start()
                if kind == "near":
                    for k, to, frm in pieces(here.core, chip, j, d, True):
                        remote(outs[k].at[to], outs[k].at[to], gat_send.at[s], gat_recv.at[s, 3 * d + j], here.target(j, d)).start()

        spread(here, own, step_fn, hook)
        sums.settle()
        spread_settle(own, sums.mine.at[0], fwd_send, fwd_recv, gat_send)
        drain(own, out_sem.at[0])

    return sums, gather


def right_scratch(n1, n2):
    unit = (n1 + n2) // 32
    return [
        *Sums.scratch(unit, RANK, 104, RANK),
        DMA((HALF,)), DMA((HALF, 6)), DMA((HALF + 1,)), DMA((HALF + 1,)), DMA((1,)),
    ]


RS_SLOTS = 2 * (HALF - 1)
AG_SLOTS = 2 * (HALF - 2)


def power_right(ins, outs, refs):
    a_up, b_up, p_up, a_dn, b_dn, p_dn = ins
    q_up, q_dn = outs
    (a1_v, p1_v, a2_v, p2_v, u_v, b_v, q_v, a_sem, p_sem, b_sem, q_sem) = refs
    plan = []
    for k, (a, p, a_v, p_v) in enumerate(((a_dn, p_dn, a1_v, p1_v), (a_up, p_up, a2_v, p2_v))):
        cols = p_v.shape[1]

        def resident(a=a, a_v=a_v, k=k):
            return pltpu.make_async_copy(a, a_v, a_sem.at[k])

        def load(i, p=p, p_v=p_v, k=k, cols=cols):
            rows = pl.ds(pl.multiple_of(i * cols, cols), cols)
            return pltpu.make_async_copy(p.at[rows], p_v.at[lax.rem(i, 2)], p_sem.at[k, lax.rem(i, 2)])

        def compute(i, a_v=a_v, p_v=p_v, k=k, cols=cols):
            at = pl.ds(pl.multiple_of(i * cols, cols), cols)
            u_v[k, :, at] = mat_nt(a_v[...], p_v[lax.rem(i, 2)]).astype(BF16)

        plan.append((Phase(RANK // cols, (load,), compute, resident=(resident,)), 1))
    for k, (b, q, rate) in enumerate(((b_dn, q_dn, 4), (b_up, q_up, 4))):
        def load(i, b=b, k=k):
            cols = pl.ds(pl.multiple_of(i * TILE, TILE), TILE)
            return pltpu.make_async_copy(b.at[:, cols], b_v.at[lax.rem(i, 3)], b_sem.at[k, lax.rem(i, 3)])

        def store(i, q=q, k=k):
            rows = pl.ds(pl.multiple_of(i * TILE, TILE), TILE)
            return pltpu.make_async_copy(q_v.at[k, lax.rem(i, 3)], q.at[rows], q_sem.at[k, lax.rem(i, 3)])

        def compute(i, k=k):
            q_v[k, lax.rem(i, 3)] = mat_nn(b_v[lax.rem(i, 3)].T, u_v[k])

        plan.append((Phase(b.shape[1] // TILE, (load,), compute, stores=(store,), depth=3), rate))
    return Background(plan)


def power_right_scratch(m1, m2):
    return [
        pltpu.VMEM((RANK, m2), BF16), pltpu.VMEM((2, TILE, m2), BF16),
        pltpu.VMEM((RANK, m1), BF16), pltpu.VMEM((2, TILE, m1), BF16),
        pltpu.VMEM((2, RANK, RANK), BF16), pltpu.VMEM((3, RANK, TILE), BF16), pltpu.VMEM((2, 3, TILE, RANK), F32),
        DMA((2,)), DMA((2, 2)), DMA((2, 3)), DMA((2, 3)),
    ]


def split_at(refs, *counts):
    out = []
    for c in counts:
        out.append(refs[:c])
        refs = refs[c:]
    return (*out, refs)


def sds(shape, dtype):
    return jax.ShapeDtypeStruct(shape, dtype)


def comm_params(number):
    return pltpu.CompilerParams(collective_id=number, has_side_effects=True, vmem_limit_bytes=67043328)


def tile(i, size):
    return pl.ds(pl.multiple_of(i * size, size), size)


def cot_phases(ins, outs, keep, refs):
    g, w, z, q, a = ins
    e_out, p_out = outs
    g_v, w_v, z_v, q_v, e_v, acc, g_sem, w_sem, z_sem, q_sem, e_sem, s_v, a_v, p_v, a_sem, p_sem = refs
    count = z.shape[1] // TILE

    def resident():
        return pltpu.make_async_copy(g, g_v, g_sem.at[0])

    def w_load(i):
        return pltpu.make_async_copy(w.at[tile(i, TILE)], w_v.at[lax.rem(i, COT_DEPTH)], w_sem.at[lax.rem(i, COT_DEPTH)])

    def z_load(i):
        return pltpu.make_async_copy(z.at[:, tile(i, TILE)], z_v.at[lax.rem(i, COT_DEPTH)], z_sem.at[lax.rem(i, COT_DEPTH)])

    def q_load(i):
        return pltpu.make_async_copy(q.at[tile(i, TILE)], q_v.at[lax.rem(i, COT_DEPTH)], q_sem.at[lax.rem(i, COT_DEPTH)])

    def e_store(i):
        return pltpu.make_async_copy(e_v.at[lax.rem(i, COT_DEPTH)], e_out.at[:, tile(i, TILE)], e_sem.at[lax.rem(i, COT_DEPTH)])

    def cot(i):
        s = lax.rem(i, COT_DEPTH)
        e = gelu_grad(z_v[s].astype(F32), mat_nt(g_v[...], w_v[s])).astype(BF16)
        e_v[s] = e
        if keep is not None:
            keep[:, tile(i, TILE)] = e
        part = mat_nn(e, q_v[s])

        @pl.when(i == 0)
        def _():
            acc[...] = part

        @pl.when(i > 0)
        def _():
            acc[...] += part

        @pl.when(i == count - 1)
        def _():
            s_v[...] = acc[...].astype(BF16).T

    return (
        Phase(count, (w_load, z_load, q_load), cot, stores=(e_store,), resident=(resident,), depth=COT_DEPTH),
        p_phase(a, p_out, s_v, a_v, p_v, a_sem, p_sem),
    )


def p_phase(a, p_out, s_v, a_v, p_v, a_sem, p_sem):
    def load(i):
        return pltpu.make_async_copy(a.at[:, tile(i, TILE)], a_v.at[lax.rem(i, 4)], a_sem.at[lax.rem(i, 4)])

    def store(i):
        return pltpu.make_async_copy(p_v.at[lax.rem(i, 4)], p_out.at[:, tile(i, TILE)], p_sem.at[lax.rem(i, 4)])

    def compute(i):
        p_v[lax.rem(i, 4)] = mat_nn(s_v[...], a_v[lax.rem(i, 4)])

    return Phase(a.shape[1] // TILE, (load,), compute, stores=(store,), depth=4)


def p_scratch():
    return [pltpu.VMEM((RANK, RANK), BF16), pltpu.VMEM((4, RANK, TILE), BF16), pltpu.VMEM((4, RANK, TILE), F32), DMA((4,)), DMA((4,))]


def cot_scratch(m):
    sems = DMA((COT_DEPTH,))
    return [
        pltpu.VMEM((RANK, m), BF16), pltpu.VMEM((COT_DEPTH, TILE, m), BF16), pltpu.VMEM((COT_DEPTH, RANK, TILE), BF16), pltpu.VMEM((COT_DEPTH, TILE, RANK), BF16),
        pltpu.VMEM((COT_DEPTH, RANK, TILE), BF16), pltpu.VMEM((RANK, RANK), F32), sems, sems, sems, sems, sems, *p_scratch(),
    ]


def grad_phases(ins, outs, e_full, dy_v, refs):
    w, q, a = ins
    g_out, p_out = outs
    w_v, g_v, q_v, w_sem, g_sem, q_sem, s_v, a_v, p_v, a_sem, p_sem = refs
    m = g_v.shape[1]

    def w_load(i):
        return pltpu.make_async_copy(w.at[tile(i, TILE)], w_v.at[lax.rem(i, 2)], w_sem.at[lax.rem(i, 2)])

    def g_store(i):
        return pltpu.make_async_copy(g_v.at[:, tile(i, TILE)], g_out.at[:, tile(i, TILE)], g_sem.at[lax.rem(i, 2)])

    def grad(i):
        at = tile(i, TILE)
        g_v[:, at] = (dy_v[:, at].astype(F32) + mat_nt(e_full[...], w_v[lax.rem(i, 2)])).astype(BF16)

    def q_load(i):
        return pltpu.make_async_copy(q.at[:, tile(i, TILE)], q_v.at[lax.rem(i, 2)], q_sem.at[lax.rem(i, 2)])

    def sketch(i):
        s_v[tile(i, TILE)] = mat_nn(g_v[...], q_v[lax.rem(i, 2)]).astype(BF16).T

    return (
        Phase(m // TILE, (w_load,), grad, stores=(g_store,)),
        Phase(2, (q_load,), sketch),
        p_phase(a, p_out, s_v, a_v, p_v, a_sem, p_sem),
    )


def grad_scratch(m, n):
    two = DMA((2,))
    return [
        pltpu.VMEM((2, TILE, n), BF16), pltpu.VMEM((RANK, m), BF16), pltpu.VMEM((2, m, TILE), BF16), two, two, two,
    ]


def left_kernel(m1, p_ref, p_up, cot, after, outs, comm):
    here = Place()
    here.barrier()
    count = len(Sums.scratch(16, LANES, 16, LANES))
    sums_dn = left_sums(here, p_ref, comm[:count])
    sums_up = left_sums(here, p_up, comm[count : 2 * count])
    normalise, gather = left_gather(here, m1, outs, comm[2 * count :])
    sums_dn.start()
    cot.begin()
    after.begin()
    own = sums_dn.run(cot.run)
    cot.end(RS_SLOTS)
    sums_up.start()
    normalise(own, m1)
    own = sums_up.run(after.run)
    normalise(own, 0)
    copies = gather(lambda s: after.run(RS_SLOTS + s))
    after.end(RS_SLOTS + AG_SLOTS)
    sums_dn.settle()
    sums_up.settle()
    for copy in copies:
        copy.wait()


def left_scratch(m1, m2):
    return [*left_sums_scratch(m2), *left_sums_scratch(m1), *left_gather_scratch(m1 + m2)]


def left_grad_kernel(m, n, n_comm, layer, *refs):
    ins, outs, comm, work = split_at(refs, 9, 6, n_comm)
    p_ref, dy, w_down, z, q_up, h, w_up, q_down, a = ins
    phat_up, phat_dn, e_out, p_up, g_out, p_dn = outs
    e_full, *work = work
    n_cot = len(cot_scratch(m))
    cot = cot_phases((dy, w_down.at[layer], z, q_up.at[layer], h), (e_out, p_up), e_full, work[:n_cot])
    grad = grad_phases((w_up.at[layer], q_down.at[layer - 1], a), (g_out, p_dn), e_full, work[0], [*work[n_cot:], *work[n_cot - 5 : n_cot]])
    left_kernel(m, p_ref, p_up, Background(list(zip(cot, K1_RATES[:2]))), Background(list(zip(grad, K1_RATES[2:]))), (phat_up, phat_dn), comm)


def left_grad(p_dn, dy, w_down, z, q_up, h, w_up, q_down, a, layer):
    rank, n = p_dn.shape
    tokens, m = dy.shape
    comm = left_scratch(m, n)
    return pl.pallas_call(
        functools.partial(left_grad_kernel, m, n, len(comm), layer),
        out_shape=(sds((rank, m), BF16), sds((rank, n), BF16), sds((tokens, n), BF16), sds((rank, m), F32), sds((tokens, m), BF16), sds((rank, n), F32)),
        in_specs=[ANY] * 9,
        out_specs=(ANY,) * 6,
        scratch_shapes=comm + [pltpu.VMEM((tokens, n), BF16)] + cot_scratch(m) + grad_scratch(m, n),
        compiler_params=comm_params(0),
        name="left_grad",
    )(p_dn, dy, w_down, z, q_up, h, w_up, q_down, a)


def left_right_kernel(m, n, n_comm, layer, *refs):
    ins, work_ins, outs, comm, work = split_at(refs, 6, 6, 6, n_comm)
    p_ref, g, w_down, z, q_up, a = ins
    phat_up, phat_dn, e_out, p_up, *q_out = outs
    n_cot = len(cot_scratch(m))
    cot = cot_phases((g, w_down.at[layer], z, q_up.at[layer], a), (e_out, p_up), None, work[:n_cot])
    right = power_right(work_ins, q_out, work[n_cot:])
    left_kernel(m, p_ref, p_up, Background(list(zip(cot, K1_RATES[:2]))), right, (phat_up, phat_dn), comm)


def left_right(p_dn, g, w_down, z, q_up, a, work, layer):
    rank, n = p_dn.shape
    tokens, m = g.shape
    a_up, b_up, _, a_dn, b_dn, _ = work
    comm = left_scratch(m, n)
    return pl.pallas_call(
        functools.partial(left_right_kernel, m, n, len(comm), layer),
        out_shape=(sds((rank, m), BF16), sds((rank, n), BF16), sds((tokens, n), BF16), sds((rank, m), F32), sds((b_up.shape[1], rank), F32), sds((b_dn.shape[1], rank), F32)),
        in_specs=[ANY] * 12,
        out_specs=(ANY,) * 6,
        scratch_shapes=comm + cot_scratch(m) + power_right_scratch(a_up.shape[1], a_dn.shape[1]),
        compiler_params=comm_params(1),
        name="left_right",
    )(p_dn, g, w_down, z, q_up, a, *work)


def right_right_kernel(n1, n2, n_comm, *refs):
    ins, work_ins, outs, work_outs, comm, work = split_at(refs, 2, 6, 2, 2, n_comm)
    here = Place()
    here.barrier()
    sums, gather = right_comm(here, n1, n2, ins, outs, comm)
    sums.start()
    back = power_right(work_ins, work_outs, work)
    back.begin()
    own = sums.run(back.run)
    gather(own, lambda s: back.run(RS_SLOTS + s))
    back.end(RS_SLOTS + AG_SLOTS)


def right_right(q1, q2, work):
    n1, rank = q1.shape
    n2 = q2.shape[0]
    a_up, b_up, _, a_dn, b_dn, _ = work
    comm = right_scratch(n1, n2)
    return pl.pallas_call(
        functools.partial(right_right_kernel, n1, n2, len(comm)),
        out_shape=(sds((n1, rank), F32), sds((n2, rank), F32), sds((b_up.shape[1], rank), F32), sds((b_dn.shape[1], rank), F32)),
        in_specs=[ANY] * 8,
        out_specs=(ANY,) * 4,
        scratch_shapes=comm + power_right_scratch(a_up.shape[1], a_dn.shape[1]),
        compiler_params=comm_params(2),
        name="right_right",
    )(q1, q2, *work)


def turn_phase(p, out, refs):
    p_v, o_v, p_sem, o_sem = refs

    def load(i):
        return pltpu.make_async_copy(p.at[:, tile(i, TILE)], p_v.at[lax.rem(i, TURN_DEPTH)], p_sem.at[lax.rem(i, TURN_DEPTH)])

    def store(i):
        return pltpu.make_async_copy(o_v.at[lax.rem(i, TURN_DEPTH)], out.at[tile(i, TILE)], o_sem.at[lax.rem(i, TURN_DEPTH)])

    def compute(i):
        o_v[lax.rem(i, TURN_DEPTH)] = p_v[lax.rem(i, TURN_DEPTH)].T

    return Phase(p.shape[1] // TILE, (load,), compute, stores=(store,), depth=TURN_DEPTH)


def turn_scratch():
    sems = DMA((TURN_DEPTH,))
    return [pltpu.VMEM((TURN_DEPTH, RANK, TILE), BF16), pltpu.VMEM((TURN_DEPTH, TILE, RANK), BF16), sems, sems]


def right_turn_kernel(n1, n2, n_comm, n_turn, *refs):
    ins, flat, outs, turned, comm, work = split_at(refs, 2, n_turn, 2, n_turn, n_comm)
    here = Place()
    here.barrier()
    sums, gather = right_comm(here, n1, n2, ins, outs, comm)
    sums.start()
    each = len(work) // n_turn
    back = Background([(turn_phase(p, out, work[k * each : (k + 1) * each]), TURN_RATE) for k, (p, out) in enumerate(zip(flat, turned))])
    back.begin()
    own = sums.run(back.run)
    gather(own, lambda s: back.run(RS_SLOTS + s))
    back.end(RS_SLOTS + AG_SLOTS)


def right_turn(q1, q2, flat):
    n1, rank = q1.shape
    n2 = q2.shape[0]
    comm = right_scratch(n1, n2)
    return pl.pallas_call(
        functools.partial(right_turn_kernel, n1, n2, len(comm), len(flat)),
        out_shape=(sds((n1, rank), F32), sds((n2, rank), F32), *(sds(p.shape[::-1], BF16) for p in flat)),
        in_specs=[ANY] * (2 + len(flat)),
        out_specs=(ANY,) * (2 + len(flat)),
        scratch_shapes=comm + turn_scratch() * len(flat),
        compiler_params=comm_params(3),
        name="right_turn",
    )(q1, q2, *flat)


def update_kernel(step_size, layer, size, slots, lead, p_ref, q_ref, w_ref, *refs):
    o_ref, qo_ref, p_rows, w_buf, q_buf, w_in, w_out, q_in, q_out, p_in = refs[-10:]
    m = p_ref.shape[0]
    blocks = q_ref.shape[0] // size

    def cols(i):
        return pl.ds(pl.multiple_of(i * size, size), size)

    def w_load(i):
        return pltpu.make_async_copy(w_ref.at[layer, :, cols(i)], w_buf.at[lax.rem(i, slots)], w_in.at[lax.rem(i, slots)])

    def q_load(i):
        return pltpu.make_async_copy(q_ref.at[cols(i)], q_buf.at[lax.rem(i, slots)], q_in.at[lax.rem(i, slots)])

    def w_store(i):
        return pltpu.make_async_copy(w_buf.at[lax.rem(i, slots)], o_ref.at[layer, :, cols(i)], w_out.at[lax.rem(i, slots)])

    def q_store(i):
        return pltpu.make_async_copy(q_buf.at[lax.rem(i, slots)], qo_ref.at[layer, cols(i)], q_out.at[lax.rem(i, slots)])

    for i in range(lead):
        w_load(i).start()
        q_load(i).start()
    whole = pltpu.make_async_copy(p_ref, p_rows, p_in.at[0])
    whole.start()
    whole.wait()

    def block(i):
        s = lax.rem(i, slots)
        q_load(i).wait()
        q_store(i).start()
        q = q_buf[s].astype(BF16)
        w_load(i).wait()
        for r in range(0, m, TILE):
            prod = mat_nt(p_rows[pl.ds(r, TILE)], q)
            w_buf[s, pl.ds(r, TILE)] = (w_buf[s, pl.ds(r, TILE)].astype(F32) - step_size * prod).astype(BF16)
        w_store(i).start()
        after = i + lead

        @pl.when(after < blocks)
        def _():
            @pl.when(after >= slots)
            def _():
                w_store(after - slots).wait()
                q_store(after - slots).wait()

            w_load(after).start()
            q_load(after).start()

    loop(0, blocks, block)

    def finish(i):
        w_store(i).wait()
        q_store(i).wait()

    loop(max(0, blocks - slots), blocks, finish)


def update(p_hat, q_sum, weights, layer, prev, step_size):
    layers, m, n = weights.shape
    rank = p_hat.shape[1]
    size = TILE
    slots, lead = (12, 6) if m < n else (6, 4)
    args = [p_hat, q_sum, weights]
    alias = {}
    if prev is not None:
        args += prev
        alias = {3: 0, 4: 1}
    dma = DMA((slots,))
    return pl.pallas_call(
        functools.partial(update_kernel, step_size, layer, size, slots, lead),
        out_shape=(sds(weights.shape, BF16), sds((layers, n, rank), F32)),
        in_specs=[ANY] * len(args),
        out_specs=(ANY,) * 2,
        scratch_shapes=[
            pltpu.VMEM((m, rank), BF16),
            pltpu.VMEM((slots, m, size), BF16),
            pltpu.VMEM((slots, size, rank), F32),
            dma, dma, dma, dma, DMA((1,)),
        ],
        input_output_aliases=alias,
        compiler_params=pltpu.CompilerParams(vmem_limit_bytes=60 * 2**20),
        cost_estimate=pl.CostEstimate(flops=2 * m * n * rank, bytes_accessed=4 * m * n, transcendentals=0),
        name="update",
    )(*args)


def residual_kernel(x_ref, a_ref, w_ref, o_ref):
    o_ref[...] = (x_ref[...].astype(F32) + mat_nn(a_ref[...], w_ref[0])).astype(BF16)


def residual(x, a, weights, layer):
    tokens, m = x.shape
    n = a.shape[1]
    block = pl.BlockSpec((tokens, TILE), lambda i: (0, i))
    return pl.pallas_call(
        residual_kernel,
        grid=(m // TILE,),
        out_shape=sds(x.shape, BF16),
        in_specs=[block, pl.BlockSpec((tokens, n), lambda i: (0, 0)), pl.BlockSpec((1, n, TILE), lambda i: (layer, 0, i))],
        out_specs=block,
        compiler_params=pltpu.CompilerParams(vmem_limit_bytes=60 * 2**20),
        cost_estimate=pl.CostEstimate(flops=2 * tokens * m * n, bytes_accessed=2 * m * n, transcendentals=0),
        name="residual",
    )(x, a, weights)


def solution(mesh):
    def left(right_in, left_in, q_fac):
        sketch = mat_nn(right_in, q_fac).astype(BF16)
        return mat_tn(sketch, left_in)

    def local_step(tok_rows, grad_rows, w_up, w_down, q_up, q_down):
        step_size = 0.4 / math.sqrt(q_up.shape[-1])
        z0 = mat_nn(tok_rows, w_up[0]).astype(BF16)
        a0 = gelu_tanh(z0.astype(F32)).astype(BF16)
        h1 = residual(tok_rows, a0, w_down, 0)
        z1 = mat_nn(h1, w_up[1]).astype(BF16)
        a1 = gelu_tanh(z1.astype(F32)).astype(BF16)
        pu1, pd1, e1, _, g1, pd0_part = left_grad(left(grad_rows, a1, q_down[1]), grad_rows, w_down, z1, q_up, h1, w_up, q_down, a0, 1)
        pu0, pd0, e0, _, qu1, qd1 = left_right(pd0_part, g1, w_down, z0, q_up, tok_rows, (h1, e1, pu1, a1, grad_rows, pd1), 0)
        qu1, qd1, qu0, qd0 = right_right(qu1, qd1, (tok_rows, e0, pu0, a0, g1, pd0))
        qu0, qd0, pu1, pd1, pu0, pd0 = right_turn(qu0, qd0, (pu1, pd1, pu0, pd0))
        up = update(pu1, qu1, w_up, 1, None, step_size)
        down = update(pd1, qd1, w_down, 1, None, step_size)
        up = update(pu0, qu0, w_up, 0, up, step_size)
        down = update(pd0, qd0, w_down, 0, down, step_size)
        return up[0], down[0], up[1], down[1]

    row_spec = P(mesh.axis_names[0], None)
    return jax.shard_map(local_step, mesh=mesh, in_specs=(row_spec, row_spec, P(), P(), P(), P()), out_specs=(P(), P(), P(), P()), check_vma=False)
```

```python
import math
import functools
import jax
import jax.numpy as jnp
from jax import lax
from jax.experimental import pallas as pl
from jax.experimental.pallas import tpu as pltpu
from jax.sharding import PartitionSpec as P

MESH = pl.DeviceIdType.MESH
DMA = pltpu.SemaphoreType.DMA
ANY = pl.BlockSpec(memory_space=pl.ANY)
F32, BF16 = jnp.float32, jnp.bfloat16
CYCLES = (
    (0, 1, 3, 2, 6, 7, 5, 9, 11, 10, 14, 15, 13, 12, 8, 4),
    (0, 1, 5, 4, 6, 10, 8, 9, 13, 12, 14, 15, 11, 7, 3, 2),
    (0, 2, 6, 7, 3, 1, 5, 9, 13, 15, 11, 10, 14, 12, 8, 4),
)
TILE, RANK, LANES = 256, 512, 128
CHIPS = 16
HALF = CHIPS // 2
WINDOW = 4
AHEAD = 2
COT_DEPTH = 2
PACE = 2
K1_RATES = (4, 8, 1, 2, 14)
TURN_DEPTH = 3
TURN_RATE = 8


def mat_nn(left_op, right_op):
    return jnp.dot(left_op, right_op, preferred_element_type=F32)


def mat_nt(left_op, right_op):
    return lax.dot_general(left_op, right_op, (((1,), (1,)), ((), ())), preferred_element_type=F32)


def mat_tn(left_op, right_op):
    return lax.dot_general(left_op, right_op, (((0,), (0,)), ((), ())), preferred_element_type=F32)


def gelu_tanh(values):
    return jax.nn.gelu(values, approximate=True)


def gelu_grad(pre_gelu, cot_gelu):
    pull_back = jax.vjp(gelu_tanh, pre_gelu)[1]
    return pull_back(cot_gelu)[0]


def pick(table, index):
    value = jnp.int32(table[0])
    for k in range(1, len(table)):
        value = jnp.where(index == k, jnp.int32(table[k]), value)
    return value


def inverse(table):
    return tuple(table.index(k) for k in range(len(table)))


def loop(lo, hi, body):
    def run(i, carry):
        body(i)
        return carry

    lax.fori_loop(lo, hi, run, 0)


class Place:
    def __init__(self):
        me = lax.axis_index("data")
        self.core = lax.rem(me, 2)
        self.chip = lax.div(me, 2)
        self.partner = me + 1 - 2 * self.core
        self.pos = [pick(inverse(c), self.chip) for c in CYCLES]
        self.ahead = [2 * pick(c, lax.rem(p + 1, CHIPS)) + self.core for c, p in zip(CYCLES, self.pos)]
        self.behind = [2 * pick(c, lax.rem(p + CHIPS - 1, CHIPS)) + self.core for c, p in zip(CYCLES, self.pos)]

    def target(self, j, d):
        return jnp.where(d == 0, self.ahead[j], self.behind[j])

    def owner(self, j, d, back):
        p = self.pos[j]
        return pick(CYCLES[j], jnp.where(d == 0, lax.rem(p + 2 * CHIPS - back, CHIPS), lax.rem(p + 2 * CHIPS + back, CHIPS)))

    def barrier(self):
        sem = pltpu.get_barrier_semaphore()
        for dev in (*self.ahead, *self.behind, self.partner):
            pl.semaphore_signal(sem, inc=1, device_id=(dev,), device_id_type=MESH)
        pl.semaphore_wait(sem, 7)


def remote(src, dst, send, recv, dev):
    return pltpu.make_async_remote_copy(src_ref=src, dst_ref=dst, send_sem=send, recv_sem=recv, device_id=(dev,), device_id_type=MESH)


def drain(ref, sem):
    pltpu.make_async_copy(ref, ref, sem).wait()


class Phase:
    def __init__(self, count, loads, compute, stores=(), resident=(), depth=2):
        self.count, self.loads, self.compute, self.stores, self.resident, self.depth = count, loads, compute, stores, resident, depth
        self.follower = None

    def begin(self):
        for copy in self.resident:
            copy().start()
        for i in range(min(self.depth - 1, self.count)):
            for load in self.loads:
                load(i).start()

    def tile(self, i):
        if self.resident:
            @pl.when(i == 0)
            def _():
                for copy in self.resident:
                    copy().wait()

        for load in self.loads:
            load(i).wait()
        after = i + self.depth - 1

        @pl.when(after < self.count)
        def _():
            for load in self.loads:
                load(after).start()

        if self.stores:
            @pl.when(i >= self.depth)
            def _():
                for store in self.stores:
                    store(i - self.depth).wait()

        self.compute(i)
        for store in self.stores:
            store(i).start()
        if self.follower is not None:
            @pl.when(i == self.count - 1)
            def _():
                self.follower.begin()

    def end(self):
        for i in range(max(0, self.count - self.depth), self.count):
            for store in self.stores:
                store(i).wait()


class Background:
    def __init__(self, plan):
        self.plan = []
        at = 0
        for phase, rate in plan:
            slots = -(-phase.count * PACE // rate)
            self.plan.append((phase, rate, at, slots))
            at += slots
        self.slots = at
        for (one, *_), (other, *_) in zip(self.plan, self.plan[1:]):
            one.follower = other

    def begin(self):
        self.plan[0][0].begin()

    def run(self, slot):
        for phase, rate, at, slots in self.plan:
            lo = jnp.clip(lax.div((slot - at) * rate, PACE), 0, phase.count)
            hi = jnp.clip(lax.div((slot - at + 1) * rate, PACE), 0, phase.count)
            loop(lo, hi, phase.tile)

    def end(self, done):
        for phase, rate, at, slots in self.plan:
            lo = min(max((done - at) * rate, 0) // PACE, phase.count)
            if lo < phase.count:
                loop(lo, phase.count, phase.tile)
            phase.end()


class Sums:
    def __init__(self, here, ins, pieces, region, refs):
        self.here, self.ins, self.pieces, self.region = here, ins, pieces, region
        self.mine, self.part, self.slots, self.stage_sem, self.pair_send, self.pair_recv, self.ring_send, self.ring_recv, self.credit = refs

    @staticmethod
    def scratch(height, width, slot_rows, slot_cols):
        return [
            pltpu.VMEM((WINDOW, 2, height, width), F32),
            pltpu.VMEM((WINDOW, 2, height, width), F32),
            pltpu.VMEM((HALF, 6, slot_rows, slot_cols), F32),
            DMA((HALF + 1,)), DMA((HALF + 1,)), DMA((HALF + 1,)), DMA((HALF,)), DMA((HALF, 6)), pltpu.SemaphoreType.REGULAR,
        ]

    def units(self, sem, t, single):
        drain(self.mine.at[0, 0] if single else self.mine.at[0], sem.at[t])

    def stage(self, t, kind, reuse):
        here = self.here
        w = lax.rem(t, WINDOW)
        if reuse is not None:
            self.units(self.ring_send, t - WINDOW, reuse == "far")
            pl.semaphore_wait(self.credit, 1)
        for d in range(1 if kind == "own" else 2):
            for j in range(3):
                chip = here.owner(j, d, t - HALF)
                for k, frm, to in self.pieces(here.core, chip, j, d, kind == "far"):
                    pltpu.make_async_copy(self.ins[k].at[frm], self.mine.at[(w, d, *to)], self.stage_sem.at[t]).start()
                for k, frm, to in self.pieces(1 - here.core, chip, j, d, kind == "far"):
                    remote(self.ins[k].at[frm], self.part.at[(w, d, *to)], self.pair_send.at[t], self.pair_recv.at[t], here.partner).start()

    def send(self, block, t, d, j, height, width):
        spot = (t, 3 * d + j, pl.ds(0, height), pl.ds(0, width))
        remote(block, self.slots.at[spot], self.ring_send.at[t], self.ring_recv.at[t, 3 * d + j], self.here.target(j, d)).start()

    def come(self, t, d, j, height, width):
        slot = self.slots.at[(t, 3 * d + j, pl.ds(0, height), pl.ds(0, width))]
        drain(slot, self.ring_recv.at[t, 3 * d + j])
        return slot

    def give(self):
        pl.semaphore_signal(self.credit, inc=1, device_id=(self.here.partner,), device_id_type=MESH)

    def start(self):
        self.stage(0, "far", None)
        self.stage(1, "full", None)
        self.stage(2, "full", None)

    def first(self):
        self.units(self.stage_sem, 0, True)
        self.units(self.pair_recv, 0, True)
        for d in range(2):
            for j in range(3):
                region = (0, d, *self.region(j, d, True))
                block = self.mine.at[region]
                value = block[...] + self.part[region]
                block[...] = value
                self.send(block, 0, d, j, *value.shape)
        self.give()

    def middle(self, t, d):
        w = lax.rem(t, WINDOW)

        @pl.when(d == 0)
        def _():
            @pl.when(t == 1)
            def _():
                self.stage(t + AHEAD, "full", None)

            @pl.when(t == 2)
            def _():
                self.stage(t + AHEAD, "full", "far")

            @pl.when((t > 2) & (t + AHEAD < HALF))
            def _():
                self.stage(t + AHEAD, "full", "full")

            @pl.when(t + AHEAD == HALF)
            def _():
                self.stage(t + AHEAD, "own", "full")

            self.units(self.stage_sem, t, False)
            self.units(self.pair_recv, t, False)

        for j in range(3):
            region = (w, d, *self.region(j, 0, False))
            block = self.mine.at[region]
            height, width = block.shape

            @pl.when(t == 1)
            def _():
                block[...] = block[...] + self.part[region]
                for side in range(2):
                    @pl.when(d == side)
                    def _():
                        half = self.region(j, side, True)
                        some = self.mine.at[(w, d, *half)]
                        slot = self.come(0, d, j, *some.shape)
                        some[...] = some[...] + slot[...]

            @pl.when(t > 1)
            def _():
                slot = self.come(t - 1, d, j, height, width)
                block[...] = block[...] + self.part[region] + slot[...]

            self.send(block, t, d, j, height, width)

        @pl.when((d == 1) & (t + WINDOW <= HALF))
        def _():
            self.give()

    def last(self):
        self.units(self.stage_sem, HALF, True)
        self.units(self.pair_recv, HALF, True)
        own = self.mine.at[HALF % WINDOW, 0]
        for j in range(3):
            region = self.region(j, 0, False)
            block = own.at[region]
            height, width = block.shape
            value = block[...] + self.part[(HALF % WINDOW, 0, *region)]
            for d in range(2):
                value = value + self.come(HALF - 1, d, j, height, width)[...]
            block[...] = value
        return own

    def run(self, hook):
        self.first()

        def body(u):
            self.middle(lax.div(u, 2), lax.rem(u, 2))
            if hook is not None:
                hook(u - 2)

        loop(2, 2 * HALF, body)
        return self.last()

    def settle(self):
        def pairs(t):
            self.units(self.pair_send, t, False)

        self.units(self.pair_send, 0, True)
        loop(1, HALF, pairs)
        self.units(self.pair_send, HALF, True)
        loop(HALF + 1 - WINDOW, HALF, lambda t: self.units(self.ring_send, t, False))


def spread(here, unit, step_fn, hook):
    step_fn(0, 0, "own")

    def body(u):
        step_fn(lax.div(u, 2), lax.rem(u, 2), "full")
        if hook is not None:
            hook(u - 2)

    loop(2, 2 * (HALF - 1), body)
    for d in range(2):
        step_fn(HALF - 1, d, "near")
    for d in range(2):
        step_fn(HALF, d, "far")


def spread_settle(unit, pair, fwd_send, fwd_recv, gat_send):
    def both(sem, s, single):
        drain(unit if single else pair, sem.at[s])

    for sem in (fwd_recv, fwd_send):
        both(sem, 0, True)
        loop(1, HALF, lambda s, sem=sem: both(sem, s, False))
        both(sem, HALF, True)
    loop(0, HALF - 1, lambda s: both(gat_send, s, False))
    both(gat_send, HALF - 1, True)


def left_sums(here, p_ref, refs):
    width = p_ref.shape[1]
    tiles = width // LANES
    third = (tiles + 2) // 3
    second = (tiles - third + 1) // 2
    cuts = (0, LANES * third, LANES * (third + second), width)

    def region(j, d, far):
        return pl.ds(8 * d if far else 0, 8 if far else 16), pl.ds(cuts[j], cuts[j + 1] - cuts[j])

    def pieces(core, chip, j, d, far):
        row = pl.multiple_of(TILE * core + 16 * chip + (8 * d if far else 0), 8)
        rows, cols = region(j, d, far)
        return ((0, (pl.ds(row, 8 if far else 16), cols), (rows, cols)),)

    return Sums(here, (p_ref,), pieces, region, refs)


def left_sums_scratch(width):
    return Sums.scratch(16, width, 16, (width // LANES + 2) // 3 * LANES)


def left_gather(here, m1, outs, refs):
    phat, gat_send, gat_recv, fwd_send, fwd_recv, out_sem = refs
    width = phat.shape[1]
    third = (width // LANES + 2) // 3 * LANES
    cuts = (0, third, 2 * third, width)

    def normalise(own, lo):
        rows = pl.ds(pl.multiple_of(TILE * here.core + 16 * here.chip, 16), 16)
        total = jnp.zeros((16, LANES), F32)
        for c in range(0, own.shape[1], LANES):
            v = own[:, pl.ds(c, LANES)]
            total = total + v * v
        norm = jnp.sqrt(jnp.sum(total, axis=1, keepdims=True))
        for c in range(0, own.shape[1], TILE):
            phat[rows, pl.ds(lo + c, TILE)] = (own[:, pl.ds(c, TILE)] / norm).astype(BF16)

    def step_fn(s, d, kind):
        for j in range(3):
            start, size = cuts[j], cuts[j + 1] - cuts[j]
            mid = (size // LANES + 1) // 2 * LANES
            halves = (pl.ds(start, mid), pl.ds(start + mid, size - mid))
            rows = pl.ds(pl.multiple_of(TILE * here.core + 16 * here.owner(j, d, s), 16), 16)
            block = phat.at[rows, pl.ds(start, size)]
            if kind == "far":
                block = phat.at[rows, halves[d]]
            if kind != "own":
                drain(block, gat_recv.at[s - 1, 3 * d + j])
            onward = ()
            if kind == "own":
                onward = ((0, block), (1, block))
            elif kind == "full":
                onward = ((d, block),)
            elif kind == "near":
                onward = ((d, phat.at[rows, halves[d]]),)
            for way, some in onward:
                remote(some, some, gat_send.at[s], gat_recv.at[s, 3 * way + j], here.target(j, way)).start()
            remote(block, block, fwd_send.at[s], fwd_recv.at[s], here.partner).start()

    def gather(hook):
        unit = phat.at[pl.ds(0, 16)]
        spread(here, unit, step_fn, hook)
        spread_settle(unit, phat.at[pl.ds(0, 32)], fwd_send, fwd_recv, gat_send)
        copies = [
            pltpu.make_async_copy(phat.at[:, pl.ds(0, m1)], outs[0], out_sem.at[0]),
            pltpu.make_async_copy(phat.at[:, pl.ds(m1, width - m1)], outs[1], out_sem.at[1]),
        ]
        for copy in copies:
            copy.start()
        return copies

    return normalise, gather


def left_gather_scratch(width):
    return [
        pltpu.VMEM((RANK, width), BF16),
        DMA((HALF,)), DMA((HALF, 6)), DMA((HALF + 1,)), DMA((HALF + 1,)), DMA((2,)),
    ]


def right_comm(here, n1, n2, ins, outs, refs):
    *sum_refs, gat_send, gat_recv, fwd_send, fwd_recv, out_sem = refs
    u1, u2 = n1 // 32, n2 // 32
    w1 = u1 // 3
    second = (u2 - 16) // 16 * 8
    w2 = (u2 - 2 * second, second, second)
    from2 = (0, w2[0], w2[0] + second)
    sizes = tuple(w1 + w2[j] for j in range(3))
    offs = (0, sizes[0], sizes[0] + sizes[1])

    def columns(d, far):
        return pl.ds(TILE * d if far else 0, TILE if far else RANK)

    def region(j, d, far):
        return pl.ds(offs[j], sizes[j]), columns(d, far)

    def pieces(core, chip, j, d, far):
        cols = columns(d, far)
        row1 = pl.multiple_of((n1 // 2) * core + u1 * chip + w1 * j, 8)
        row2 = pl.multiple_of((n2 // 2) * core + u2 * chip + from2[j], 8)
        return (
            (0, (pl.ds(row1, w1), cols), (pl.ds(offs[j], w1), cols)),
            (1, (pl.ds(row2, w2[j]), cols), (pl.ds(offs[j] + w1, w2[j]), cols)),
        )

    sums = Sums(here, ins, pieces, region, sum_refs)

    def gather(own, hook):
        def step_fn(s, d, kind):
            for j in range(3):
                chip = here.owner(j, d, s)
                if kind != "own":
                    drain(own.at[pl.ds(0, sizes[j]), columns(0, kind == "far")], gat_recv.at[s - 1, 3 * d + j])
                for k, to, frm in pieces(here.core, chip, j, d, kind == "far"):
                    dst = outs[k].at[to]
                    src = own.at[frm] if kind == "own" else dst
                    if kind == "own":
                        pltpu.make_async_copy(src, dst, out_sem.at[0]).start()
                    for way in {"own": (0, 1), "full": (d,)}.get(kind, ()):
                        remote(src, dst, gat_send.at[s], gat_recv.at[s, 3 * way + j], here.target(j, way)).start()
                    remote(src, dst, fwd_send.at[s], fwd_recv.at[s], here.partner).start()
                if kind == "near":
                    for k, to, frm in pieces(here.core, chip, j, d, True):
                        remote(outs[k].at[to], outs[k].at[to], gat_send.at[s], gat_recv.at[s, 3 * d + j], here.target(j, d)).start()

        spread(here, own, step_fn, hook)
        sums.settle()
        spread_settle(own, sums.mine.at[0], fwd_send, fwd_recv, gat_send)
        drain(own, out_sem.at[0])

    return sums, gather


def right_scratch(n1, n2):
    unit = (n1 + n2) // 32
    return [
        *Sums.scratch(unit, RANK, 104, RANK),
        DMA((HALF,)), DMA((HALF, 6)), DMA((HALF + 1,)), DMA((HALF + 1,)), DMA((1,)),
    ]


RS_SLOTS = 2 * (HALF - 1)
AG_SLOTS = 2 * (HALF - 2)


def power_right(ins, outs, refs):
    a_up, b_up, p_up, a_dn, b_dn, p_dn = ins
    q_up, q_dn = outs
    (a1_v, p1_v, a2_v, p2_v, u_v, b_v, q_v, a_sem, p_sem, b_sem, q_sem) = refs
    plan = []
    for k, (a, p, a_v, p_v) in enumerate(((a_dn, p_dn, a1_v, p1_v), (a_up, p_up, a2_v, p2_v))):
        cols = p_v.shape[1]

        def resident(a=a, a_v=a_v, k=k):
            return pltpu.make_async_copy(a, a_v, a_sem.at[k])

        def load(i, p=p, p_v=p_v, k=k, cols=cols):
            rows = pl.ds(pl.multiple_of(i * cols, cols), cols)
            return pltpu.make_async_copy(p.at[rows], p_v.at[lax.rem(i, 2)], p_sem.at[k, lax.rem(i, 2)])

        def compute(i, a_v=a_v, p_v=p_v, k=k, cols=cols):
            at = pl.ds(pl.multiple_of(i * cols, cols), cols)
            u_v[k, :, at] = mat_nt(a_v[...], p_v[lax.rem(i, 2)]).astype(BF16)

        plan.append((Phase(RANK // cols, (load,), compute, resident=(resident,)), 1))
    for k, (b, q, rate) in enumerate(((b_dn, q_dn, 5), (b_up, q_up, 5))):
        def load(i, b=b, k=k):
            cols = pl.ds(pl.multiple_of(i * TILE, TILE), TILE)
            return pltpu.make_async_copy(b.at[:, cols], b_v.at[lax.rem(i, 3)], b_sem.at[k, lax.rem(i, 3)])

        def store(i, q=q, k=k):
            rows = pl.ds(pl.multiple_of(i * TILE, TILE), TILE)
            return pltpu.make_async_copy(q_v.at[k, lax.rem(i, 3)], q.at[rows], q_sem.at[k, lax.rem(i, 3)])

        def compute(i, k=k):
            q_v[k, lax.rem(i, 3)] = mat_nn(b_v[lax.rem(i, 3)].T, u_v[k])

        plan.append((Phase(b.shape[1] // TILE, (load,), compute, stores=(store,), depth=3), rate))
    return Background(plan)


def power_right_scratch(m1, m2):
    return [
        pltpu.VMEM((RANK, m2), BF16), pltpu.VMEM((2, TILE, m2), BF16),
        pltpu.VMEM((RANK, m1), BF16), pltpu.VMEM((2, TILE, m1), BF16),
        pltpu.VMEM((2, RANK, RANK), BF16), pltpu.VMEM((3, RANK, TILE), BF16), pltpu.VMEM((2, 3, TILE, RANK), F32),
        DMA((2,)), DMA((2, 2)), DMA((2, 3)), DMA((2, 3)),
    ]


def split_at(refs, *counts):
    out = []
    for c in counts:
        out.append(refs[:c])
        refs = refs[c:]
    return (*out, refs)


def sds(shape, dtype):
    return jax.ShapeDtypeStruct(shape, dtype)


def comm_params(number):
    return pltpu.CompilerParams(collective_id=number, has_side_effects=True, vmem_limit_bytes=67043328)


def tile(i, size):
    return pl.ds(pl.multiple_of(i * size, size), size)


def cot_phases(ins, outs, keep, refs):
    g, w, z, q, a = ins
    e_out, p_out = outs
    g_v, w_v, z_v, q_v, e_v, acc, g_sem, w_sem, z_sem, q_sem, e_sem, s_v, a_v, p_v, a_sem, p_sem = refs
    count = z.shape[1] // TILE

    def resident():
        return pltpu.make_async_copy(g, g_v, g_sem.at[0])

    def w_load(i):
        return pltpu.make_async_copy(w.at[tile(i, TILE)], w_v.at[lax.rem(i, COT_DEPTH)], w_sem.at[lax.rem(i, COT_DEPTH)])

    def z_load(i):
        return pltpu.make_async_copy(z.at[:, tile(i, TILE)], z_v.at[lax.rem(i, COT_DEPTH)], z_sem.at[lax.rem(i, COT_DEPTH)])

    def q_load(i):
        return pltpu.make_async_copy(q.at[tile(i, TILE)], q_v.at[lax.rem(i, COT_DEPTH)], q_sem.at[lax.rem(i, COT_DEPTH)])

    def e_store(i):
        return pltpu.make_async_copy(e_v.at[lax.rem(i, COT_DEPTH)], e_out.at[:, tile(i, TILE)], e_sem.at[lax.rem(i, COT_DEPTH)])

    def cot(i):
        s = lax.rem(i, COT_DEPTH)
        e = gelu_grad(z_v[s].astype(F32), mat_nt(g_v[...], w_v[s])).astype(BF16)
        e_v[s] = e
        if keep is not None:
            keep[:, tile(i, TILE)] = e
        part = mat_nn(e, q_v[s])

        @pl.when(i == 0)
        def _():
            acc[...] = part

        @pl.when(i > 0)
        def _():
            acc[...] += part

        @pl.when(i == count - 1)
        def _():
            s_v[...] = acc[...].astype(BF16).T

    return (
        Phase(count, (w_load, z_load, q_load), cot, stores=(e_store,), resident=(resident,), depth=COT_DEPTH),
        p_phase(a, p_out, s_v, a_v, p_v, a_sem, p_sem),
    )


def p_phase(a, p_out, s_v, a_v, p_v, a_sem, p_sem):
    def load(i):
        return pltpu.make_async_copy(a.at[:, tile(i, TILE)], a_v.at[lax.rem(i, 4)], a_sem.at[lax.rem(i, 4)])

    def store(i):
        return pltpu.make_async_copy(p_v.at[lax.rem(i, 4)], p_out.at[:, tile(i, TILE)], p_sem.at[lax.rem(i, 4)])

    def compute(i):
        p_v[lax.rem(i, 4)] = mat_nn(s_v[...], a_v[lax.rem(i, 4)])

    return Phase(a.shape[1] // TILE, (load,), compute, stores=(store,), depth=4)


def p_scratch():
    return [pltpu.VMEM((RANK, RANK), BF16), pltpu.VMEM((4, RANK, TILE), BF16), pltpu.VMEM((4, RANK, TILE), F32), DMA((4,)), DMA((4,))]


def cot_scratch(m):
    sems = DMA((COT_DEPTH,))
    return [
        pltpu.VMEM((RANK, m), BF16), pltpu.VMEM((COT_DEPTH, TILE, m), BF16), pltpu.VMEM((COT_DEPTH, RANK, TILE), BF16), pltpu.VMEM((COT_DEPTH, TILE, RANK), BF16),
        pltpu.VMEM((COT_DEPTH, RANK, TILE), BF16), pltpu.VMEM((RANK, RANK), F32), sems, sems, sems, sems, sems, *p_scratch(),
    ]


def grad_phases(ins, outs, e_full, dy_v, refs):
    w, q, a = ins
    g_out, p_out = outs
    w_v, g_v, q_v, w_sem, g_sem, q_sem, s_v, a_v, p_v, a_sem, p_sem = refs
    m = g_v.shape[1]

    def w_load(i):
        return pltpu.make_async_copy(w.at[tile(i, TILE)], w_v.at[lax.rem(i, 2)], w_sem.at[lax.rem(i, 2)])

    def g_store(i):
        return pltpu.make_async_copy(g_v.at[:, tile(i, TILE)], g_out.at[:, tile(i, TILE)], g_sem.at[lax.rem(i, 2)])

    def grad(i):
        at = tile(i, TILE)
        g_v[:, at] = (dy_v[:, at].astype(F32) + mat_nt(e_full[...], w_v[lax.rem(i, 2)])).astype(BF16)

    def q_load(i):
        return pltpu.make_async_copy(q.at[:, tile(i, TILE)], q_v.at[lax.rem(i, 2)], q_sem.at[lax.rem(i, 2)])

    def sketch(i):
        s_v[tile(i, TILE)] = mat_nn(g_v[...], q_v[lax.rem(i, 2)]).astype(BF16).T

    return (
        Phase(m // TILE, (w_load,), grad, stores=(g_store,)),
        Phase(2, (q_load,), sketch),
        p_phase(a, p_out, s_v, a_v, p_v, a_sem, p_sem),
    )


def grad_scratch(m, n):
    two = DMA((2,))
    return [
        pltpu.VMEM((2, TILE, n), BF16), pltpu.VMEM((RANK, m), BF16), pltpu.VMEM((2, m, TILE), BF16), two, two, two,
    ]


def left_kernel(m1, p_ref, p_up, cot, after, outs, comm):
    here = Place()
    here.barrier()
    count = len(Sums.scratch(16, LANES, 16, LANES))
    sums_dn = left_sums(here, p_ref, comm[:count])
    sums_up = left_sums(here, p_up, comm[count : 2 * count])
    normalise, gather = left_gather(here, m1, outs, comm[2 * count :])
    sums_dn.start()
    cot.begin()
    after.begin()
    own = sums_dn.run(cot.run)
    cot.end(RS_SLOTS)
    sums_up.start()
    normalise(own, m1)
    own = sums_up.run(after.run)
    normalise(own, 0)
    copies = gather(lambda s: after.run(RS_SLOTS + s))
    after.end(RS_SLOTS + AG_SLOTS)
    sums_dn.settle()
    sums_up.settle()
    for copy in copies:
        copy.wait()


def left_scratch(m1, m2):
    return [*left_sums_scratch(m2), *left_sums_scratch(m1), *left_gather_scratch(m1 + m2)]


def left_grad_kernel(m, n, n_comm, layer, *refs):
    ins, outs, comm, work = split_at(refs, 9, 6, n_comm)
    p_ref, dy, w_down, z, q_up, h, w_up, q_down, a = ins
    phat_up, phat_dn, e_out, p_up, g_out, p_dn = outs
    e_full, *work = work
    n_cot = len(cot_scratch(m))
    cot = cot_phases((dy, w_down.at[layer], z, q_up.at[layer], h), (e_out, p_up), e_full, work[:n_cot])
    grad = grad_phases((w_up.at[layer], q_down.at[layer - 1], a), (g_out, p_dn), e_full, work[0], [*work[n_cot:], *work[n_cot - 5 : n_cot]])
    left_kernel(m, p_ref, p_up, Background(list(zip(cot, K1_RATES[:2]))), Background(list(zip(grad, K1_RATES[2:]))), (phat_up, phat_dn), comm)


def left_grad(p_dn, dy, w_down, z, q_up, h, w_up, q_down, a, layer):
    rank, n = p_dn.shape
    tokens, m = dy.shape
    comm = left_scratch(m, n)
    return pl.pallas_call(
        functools.partial(left_grad_kernel, m, n, len(comm), layer),
        out_shape=(sds((rank, m), BF16), sds((rank, n), BF16), sds((tokens, n), BF16), sds((rank, m), F32), sds((tokens, m), BF16), sds((rank, n), F32)),
        in_specs=[ANY] * 9,
        out_specs=(ANY,) * 6,
        scratch_shapes=comm + [pltpu.VMEM((tokens, n), BF16)] + cot_scratch(m) + grad_scratch(m, n),
        compiler_params=comm_params(0),
        name="left_grad",
    )(p_dn, dy, w_down, z, q_up, h, w_up, q_down, a)


def left_right_kernel(m, n, n_comm, layer, *refs):
    ins, work_ins, outs, comm, work = split_at(refs, 6, 6, 6, n_comm)
    p_ref, g, w_down, z, q_up, a = ins
    phat_up, phat_dn, e_out, p_up, *q_out = outs
    n_cot = len(cot_scratch(m))
    cot = cot_phases((g, w_down.at[layer], z, q_up.at[layer], a), (e_out, p_up), None, work[:n_cot])
    right = power_right(work_ins, q_out, work[n_cot:])
    left_kernel(m, p_ref, p_up, Background(list(zip(cot, K1_RATES[:2]))), right, (phat_up, phat_dn), comm)


def left_right(p_dn, g, w_down, z, q_up, a, work, layer):
    rank, n = p_dn.shape
    tokens, m = g.shape
    a_up, b_up, _, a_dn, b_dn, _ = work
    comm = left_scratch(m, n)
    return pl.pallas_call(
        functools.partial(left_right_kernel, m, n, len(comm), layer),
        out_shape=(sds((rank, m), BF16), sds((rank, n), BF16), sds((tokens, n), BF16), sds((rank, m), F32), sds((b_up.shape[1], rank), F32), sds((b_dn.shape[1], rank), F32)),
        in_specs=[ANY] * 12,
        out_specs=(ANY,) * 6,
        scratch_shapes=comm + cot_scratch(m) + power_right_scratch(a_up.shape[1], a_dn.shape[1]),
        compiler_params=comm_params(1),
        name="left_right",
    )(p_dn, g, w_down, z, q_up, a, *work)


def right_right_kernel(n1, n2, n_comm, *refs):
    ins, work_ins, outs, work_outs, comm, work = split_at(refs, 2, 6, 2, 2, n_comm)
    here = Place()
    here.barrier()
    sums, gather = right_comm(here, n1, n2, ins, outs, comm)
    sums.start()
    back = power_right(work_ins, work_outs, work)
    back.begin()
    own = sums.run(back.run)
    gather(own, lambda s: back.run(RS_SLOTS + s))
    back.end(RS_SLOTS + AG_SLOTS)


def right_right(q1, q2, work):
    n1, rank = q1.shape
    n2 = q2.shape[0]
    a_up, b_up, _, a_dn, b_dn, _ = work
    comm = right_scratch(n1, n2)
    return pl.pallas_call(
        functools.partial(right_right_kernel, n1, n2, len(comm)),
        out_shape=(sds((n1, rank), F32), sds((n2, rank), F32), sds((b_up.shape[1], rank), F32), sds((b_dn.shape[1], rank), F32)),
        in_specs=[ANY] * 8,
        out_specs=(ANY,) * 4,
        scratch_shapes=comm + power_right_scratch(a_up.shape[1], a_dn.shape[1]),
        compiler_params=comm_params(2),
        name="right_right",
    )(q1, q2, *work)


def turn_phase(p, out, refs):
    p_v, o_v, p_sem, o_sem = refs

    def load(i):
        return pltpu.make_async_copy(p.at[:, tile(i, TILE)], p_v.at[lax.rem(i, TURN_DEPTH)], p_sem.at[lax.rem(i, TURN_DEPTH)])

    def store(i):
        return pltpu.make_async_copy(o_v.at[lax.rem(i, TURN_DEPTH)], out.at[tile(i, TILE)], o_sem.at[lax.rem(i, TURN_DEPTH)])

    def compute(i):
        o_v[lax.rem(i, TURN_DEPTH)] = p_v[lax.rem(i, TURN_DEPTH)].T

    return Phase(p.shape[1] // TILE, (load,), compute, stores=(store,), depth=TURN_DEPTH)


def turn_scratch():
    sems = DMA((TURN_DEPTH,))
    return [pltpu.VMEM((TURN_DEPTH, RANK, TILE), BF16), pltpu.VMEM((TURN_DEPTH, TILE, RANK), BF16), sems, sems]


def right_turn_kernel(n1, n2, n_comm, n_turn, *refs):
    ins, flat, outs, turned, comm, work = split_at(refs, 2, n_turn, 2, n_turn, n_comm)
    here = Place()
    here.barrier()
    sums, gather = right_comm(here, n1, n2, ins, outs, comm)
    sums.start()
    each = len(work) // n_turn
    back = Background([(turn_phase(p, out, work[k * each : (k + 1) * each]), TURN_RATE) for k, (p, out) in enumerate(zip(flat, turned))])
    back.begin()
    own = sums.run(back.run)
    gather(own, lambda s: back.run(RS_SLOTS + s))
    back.end(RS_SLOTS + AG_SLOTS)


def right_turn(q1, q2, flat):
    n1, rank = q1.shape
    n2 = q2.shape[0]
    comm = right_scratch(n1, n2)
    return pl.pallas_call(
        functools.partial(right_turn_kernel, n1, n2, len(comm), len(flat)),
        out_shape=(sds((n1, rank), F32), sds((n2, rank), F32), *(sds(p.shape[::-1], BF16) for p in flat)),
        in_specs=[ANY] * (2 + len(flat)),
        out_specs=(ANY,) * (2 + len(flat)),
        scratch_shapes=comm + turn_scratch() * len(flat),
        compiler_params=comm_params(3),
        name="right_turn",
    )(q1, q2, *flat)


def update_kernel(step_size, layer, size, slots, lead, p_ref, q_ref, w_ref, *refs):
    o_ref, qo_ref, p_rows, w_buf, q_buf, w_in, w_out, q_in, q_out, p_in = refs[-10:]
    m = p_ref.shape[0]
    blocks = q_ref.shape[0] // size

    def cols(i):
        return pl.ds(pl.multiple_of(i * size, size), size)

    def w_load(i):
        return pltpu.make_async_copy(w_ref.at[layer, :, cols(i)], w_buf.at[lax.rem(i, slots)], w_in.at[lax.rem(i, slots)])

    def q_load(i):
        return pltpu.make_async_copy(q_ref.at[cols(i)], q_buf.at[lax.rem(i, slots)], q_in.at[lax.rem(i, slots)])

    def w_store(i):
        return pltpu.make_async_copy(w_buf.at[lax.rem(i, slots)], o_ref.at[layer, :, cols(i)], w_out.at[lax.rem(i, slots)])

    def q_store(i):
        return pltpu.make_async_copy(q_buf.at[lax.rem(i, slots)], qo_ref.at[layer, cols(i)], q_out.at[lax.rem(i, slots)])

    for i in range(lead):
        w_load(i).start()
        q_load(i).start()
    whole = pltpu.make_async_copy(p_ref, p_rows, p_in.at[0])
    whole.start()
    whole.wait()

    def block(i):
        s = lax.rem(i, slots)
        q_load(i).wait()
        q_store(i).start()
        q = q_buf[s].astype(BF16)
        w_load(i).wait()
        for r in range(0, m, TILE):
            prod = mat_nt(p_rows[pl.ds(r, TILE)], q)
            w_buf[s, pl.ds(r, TILE)] = (w_buf[s, pl.ds(r, TILE)].astype(F32) - step_size * prod).astype(BF16)
        w_store(i).start()
        after = i + lead

        @pl.when(after < blocks)
        def _():
            @pl.when(after >= slots)
            def _():
                w_store(after - slots).wait()
                q_store(after - slots).wait()

            w_load(after).start()
            q_load(after).start()

    loop(0, blocks, block)

    def finish(i):
        w_store(i).wait()
        q_store(i).wait()

    loop(max(0, blocks - slots), blocks, finish)


def update(p_hat, q_sum, weights, layer, prev, step_size):
    layers, m, n = weights.shape
    rank = p_hat.shape[1]
    size = TILE
    slots, lead = (12, 6) if m < n else (6, 4)
    args = [p_hat, q_sum, weights]
    alias = {}
    if prev is not None:
        args += prev
        alias = {3: 0, 4: 1}
    dma = DMA((slots,))
    return pl.pallas_call(
        functools.partial(update_kernel, step_size, layer, size, slots, lead),
        out_shape=(sds(weights.shape, BF16), sds((layers, n, rank), F32)),
        in_specs=[ANY] * len(args),
        out_specs=(ANY,) * 2,
        scratch_shapes=[
            pltpu.VMEM((m, rank), BF16),
            pltpu.VMEM((slots, m, size), BF16),
            pltpu.VMEM((slots, size, rank), F32),
            dma, dma, dma, dma, DMA((1,)),
        ],
        input_output_aliases=alias,
        compiler_params=pltpu.CompilerParams(vmem_limit_bytes=60 * 2**20),
        cost_estimate=pl.CostEstimate(flops=2 * m * n * rank, bytes_accessed=4 * m * n, transcendentals=0),
        name="update",
    )(*args)


def residual_kernel(x_ref, a_ref, w_ref, o_ref):
    o_ref[...] = (x_ref[...].astype(F32) + mat_nn(a_ref[...], w_ref[0])).astype(BF16)


def residual(x, a, weights, layer):
    tokens, m = x.shape
    n = a.shape[1]
    block = pl.BlockSpec((tokens, TILE), lambda i: (0, i))
    return pl.pallas_call(
        residual_kernel,
        grid=(m // TILE,),
        out_shape=sds(x.shape, BF16),
        in_specs=[block, pl.BlockSpec((tokens, n), lambda i: (0, 0)), pl.BlockSpec((1, n, TILE), lambda i: (layer, 0, i))],
        out_specs=block,
        compiler_params=pltpu.CompilerParams(vmem_limit_bytes=60 * 2**20),
        cost_estimate=pl.CostEstimate(flops=2 * tokens * m * n, bytes_accessed=2 * m * n, transcendentals=0),
        name="residual",
    )(x, a, weights)


def solution(mesh):
    def left(right_in, left_in, q_fac):
        sketch = mat_nn(right_in, q_fac).astype(BF16)
        return mat_tn(sketch, left_in)

    def local_step(tok_rows, grad_rows, w_up, w_down, q_up, q_down):
        step_size = 0.4 / math.sqrt(q_up.shape[-1])
        z0 = mat_nn(tok_rows, w_up[0]).astype(BF16)
        a0 = gelu_tanh(z0.astype(F32)).astype(BF16)
        h1 = residual(tok_rows, a0, w_down, 0)
        z1 = mat_nn(h1, w_up[1]).astype(BF16)
        a1 = gelu_tanh(z1.astype(F32)).astype(BF16)
        pu1, pd1, e1, _, g1, pd0_part = left_grad(left(grad_rows, a1, q_down[1]), grad_rows, w_down, z1, q_up, h1, w_up, q_down, a0, 1)
        pu0, pd0, e0, _, qu1, qd1 = left_right(pd0_part, g1, w_down, z0, q_up, tok_rows, (h1, e1, pu1, a1, grad_rows, pd1), 0)
        qu1, qd1, qu0, qd0 = right_right(qu1, qd1, (tok_rows, e0, pu0, a0, g1, pd0))
        qu0, qd0, pu1, pd1, pu0, pd0 = right_turn(qu0, qd0, (pu1, pd1, pu0, pd0))
        up = update(pu1, qu1, w_up, 1, None, step_size)
        down = update(pd1, qd1, w_down, 1, None, step_size)
        up = update(pu0, qu0, w_up, 0, up, step_size)
        down = update(pd0, qd0, w_down, 0, down, step_size)
        return up[0], down[0], up[1], down[1]

    row_spec = P(mesh.axis_names[0], None)
    return jax.shard_map(local_step, mesh=mesh, in_specs=(row_spec, row_spec, P(), P(), P(), P()), out_specs=(P(), P(), P(), P()), check_vma=False)
```
